512 devices in a mesh: groups: 2 (over y), rows: 16 (over z), cols: 8 (over x), depth: 2 (over core).
Axes of the slice: x: 8, y: 2, z: 16, core: 2. Of those that a mesh axis runs over, the one named last changes fastest.
The devices are a block of a 8x8x16 slice.
Arguments:
- tensor: float32 [512, 128, 256], P(('groups', 'rows'), 'cols', 'depth'), parts along dimension 0, may hold values from -6 to 6
- start_one: float32 [512, 64], P(('groups', 'rows')), parts along dimension 0, may hold values from -0.375 to 0.375
- start_two: float32 [256, 64], P(('groups', 'cols')), parts along dimension 0, may hold values from -0.5 to 0.5
- start_three: float32 [512, 32], P(('groups', 'depth')), parts along dimension 0, may hold values from -0.375 to 0.375
Outputs:
- final_one: float32 [512, 64], P(('groups', 'rows')), parts along dimension 0
- final_two: float32 [256, 64], P(('groups', 'cols')), parts along dimension 0
- final_three: float32 [512, 32], P(('groups', 'depth')), parts along dimension 0
- core_tensor: float32 [128, 64, 32], P('groups'), parts along dimension 0
The draws below stay inside these ranges and needn't reach their ends.
There are 2 independent parts, one for each index of `groups`. The reference program is written for one: setup_inputs(seed, part) draws one part's arguments, and reference() takes and returns one part's arrays. A program takes and returns all parts, laid end to end along the dimension named above; each array names one. Nothing has to cross between parts.
All inputs are finite; a program needn't handle non-finite values.
Results may differ from the reference program's by a relative error of at most 0.0001.
Values sent between devices are 32-bit elements; how exact they have to be, the bound alone decides.
No kernel may reach another device: no remote copies, remote signals or barrier semaphores. Data moves between devices by JAX's collectives and lax.ppermute only.
A program may use at most 64 MiB of HBM per device.

```python
import math
import jax
import jax.numpy as jnp
from jax import lax

RANK_ONE = 64
RANK_TWO = 64
RANK_THREE = 32
SWEEPS = 1
NEWTON = 3
DIM_ONE = 256
DIM_TWO = 128
DIM_THREE = 256


def shard_levels(stream_key, shape, shards, low, high):
    def one(dim, shards_of):
        heights = jax.random.uniform(jax.random.fold_in(jax.random.fold_in(stream_key, 6), dim), (shards_of,), jnp.float32, low / len(shards), high / len(shards))
        return jnp.repeat(jnp.exp(heights), shape[dim] // shards_of).reshape((-1,) + (1,) * (len(shape) - dim - 1))

    gain = one(*shards[0])
    for cut in shards[1:]:
        gain = gain * one(*cut)
    return gain


def noise(key, shape, scale, most, pieces=(), kind=jnp.bfloat16):
    result = scale * jax.random.normal(key, shape, jnp.float32)
    if pieces:
        result = result * shard_levels(key, shape, pieces, -0.22, 0.18)
    return jnp.clip(result, -most, most).astype(kind)


def setup_inputs(seed: int = 0, part: int = 0) -> dict:
    keys = jax.random.split(jax.random.key(seed), 5)
    part_splits = jax.random.split(jax.random.fold_in(keys[4], part), 5)
    tensor = noise(part_splits[0], (DIM_ONE, DIM_TWO, DIM_THREE), 1.0, 6.0, ((0, 16), (1, 8), (2, 2)), jnp.float32)
    start_one = noise(part_splits[1], (DIM_ONE, RANK_ONE), DIM_ONE ** -0.5, 0.375, ((0, 16),), jnp.float32)
    start_two = noise(part_splits[2], (DIM_TWO, RANK_TWO), DIM_TWO ** -0.5, 0.5, ((0, 8),), jnp.float32)
    start_three = noise(part_splits[3], (DIM_THREE, RANK_THREE), DIM_THREE ** -0.5, 0.375, ((0, 2),), jnp.float32)
    return dict(tensor=tensor, start_one=start_one, start_two=start_two, start_three=start_three)


exact_mode = lax.Precision.HIGHEST

def newton_steps(matrix):
    gram_matrix = jnp.dot(matrix.T, matrix, precision=exact_mode)
    total = jnp.trace(gram_matrix) + 1e-06
    current = matrix / jnp.sqrt(total)
    gram_matrix = gram_matrix / total
    identity = jnp.eye(matrix.shape[1], dtype=jnp.float32)
    for newton_index in range(NEWTON):
        if newton_index > 0:
            gram_matrix = jnp.dot(current.T, current, precision=exact_mode)
        current = jnp.dot(current, 1.5 * identity - 0.5 * gram_matrix, precision=exact_mode)
    return current

def reference(tensor, start_one, start_two, start_three):
    first, second, third = (start_one, start_two, start_three)
    core_flat = None
    for sweep_index in range(SWEEPS):
        sectioned = jnp.einsum('ijk,jb->bik', tensor, second, precision=exact_mode)
        unfolded = jnp.einsum('bik,kc->ibc', sectioned, third, precision=exact_mode).reshape(DIM_ONE, RANK_TWO * RANK_THREE)
        core_flat = jnp.dot(first.T, unfolded, precision=exact_mode)
        first = newton_steps(jnp.dot(unfolded, core_flat.T, precision=exact_mode))
        sectioned = jnp.einsum('ijk,ia->ajk', tensor, first, precision=exact_mode)
        unfolded = jnp.einsum('ajk,kc->jac', sectioned, third, precision=exact_mode).reshape(DIM_TWO, RANK_ONE * RANK_THREE)
        core_flat = jnp.dot(second.T, unfolded, precision=exact_mode)
        second = newton_steps(jnp.dot(unfolded, core_flat.T, precision=exact_mode))
        unfolded = jnp.einsum('ajk,jb->kab', sectioned, second, precision=exact_mode).reshape(DIM_THREE, RANK_ONE * RANK_TWO)
        core_flat = jnp.dot(third.T, unfolded, precision=exact_mode)
        third = newton_steps(jnp.dot(unfolded, core_flat.T, precision=exact_mode))
    core_tensor = core_flat.reshape(RANK_THREE, RANK_ONE, RANK_TWO).transpose(1, 2, 0)
    return (first * math.sqrt(DIM_ONE), second * math.sqrt(DIM_TWO), third * math.sqrt(DIM_THREE), core_tensor)
```

```python
import math

import jax
import jax.numpy as jnp
from jax import lax
from jax.sharding import PartitionSpec as P

NEWTON = 3
LANES = 128
exact_mode = lax.Precision.HIGHEST


def mul(left, right):
    return jnp.dot(left, right, precision=exact_mode)


def from_everyone(shard, axis):
    peers = lax.axis_size(axis)
    return lax.all_to_all(
        jnp.broadcast_to(shard[None], (peers, *shard.shape)), axis, 0, 0, tiled=True
    )


def orth_factor(gram):
    total = jnp.trace(gram) + 1e-06
    gram = gram / total
    identity = jnp.eye(gram.shape[0], dtype=jnp.float32)
    factor = None
    for step in range(NEWTON):
        move = 1.5 * identity - 0.5 * gram
        factor = move if factor is None else mul(factor, move)
        if step + 1 < NEWTON:
            gram = mul(mul(move, gram), move)
    return factor / jnp.sqrt(total)


def halves_side_by_side(block):
    half = block.shape[0] // 2
    return jnp.concatenate([block[:half], block[half:]], axis=1)


def halves_stacked(blocks):
    count, half, width = blocks.shape
    width //= 2
    pairs = jnp.stack([blocks[:, :, :width], blocks[:, :, width:]], axis=1)
    return pairs.reshape(count * 2 * half, width)


def body(tensor, start_one, start_two, start_three):
    size_one, size_two, size_three = tensor.shape
    rank_one = start_one.shape[1]
    rank_two = start_two.shape[1]
    rank_three = start_three.shape[1]
    rows, cols, depth = (lax.axis_size(name) for name in ("rows", "cols", "depth"))
    row, col, level = (lax.axis_index(name) for name in ("rows", "cols", "depth"))
    length_one, length_two, length_three = size_one * rows, size_two * cols, size_three * depth
    owners = cols * depth
    slices = rank_three // owners
    flat = tensor.reshape(size_one * size_two, size_three)

    thinned = lax.dot_general(
        start_three, flat, (((0,), (1,)), ((), ())), precision=exact_mode
    ).reshape(owners, -1, LANES)
    two_packed = halves_side_by_side(start_two)
    part = two_packed.shape[0] // depth
    two_part = lax.dynamic_slice_in_dim(two_packed, level * part, part, 0)
    lines = thinned.shape[1]
    message = jnp.concatenate(
        [thinned, jnp.broadcast_to(two_part[None], (owners, *two_part.shape))], axis=1
    )
    got = lax.all_to_all(message, ("cols", "depth"), 0, 0, tiled=True)
    got = got.reshape(cols, depth, *got.shape[1:])
    own = got[:, :, :lines].sum(axis=1).reshape(cols, slices * size_one, size_two)
    own = own.transpose(1, 0, 2).reshape(slices * size_one, length_two)
    two_old = halves_stacked(got[:, :, lines:].reshape(cols, depth * part, 2 * rank_two))

    message = jnp.concatenate([own, halves_side_by_side(start_one)], axis=0)
    got = from_everyone(message, "rows")
    whole = [
        got[:, c * size_one : (c + 1) * size_one].reshape(length_one, length_two)
        for c in range(slices)
    ]
    one_old = halves_stacked(got[:, slices * size_one :])

    unfolded = jnp.concatenate([mul(matrix, two_old) for matrix in whole], axis=1)
    core = mul(one_old.T, unfolded)
    z_part = mul(core, unfolded.T)
    z_part = lax.all_gather(z_part, "depth").sum(axis=0)
    z_one = from_everyone(z_part, "cols").sum(axis=0)
    one = mul(orth_factor(mul(z_one, z_one.T)), z_one)

    projected = jnp.concatenate([mul(one, matrix) for matrix in whole], axis=0)
    projected = from_everyone(projected, "cols").reshape(-1, length_two)
    core = mul(projected, two_old)
    z_part = mul(core.T, projected)
    z_two = lax.all_gather(z_part, "depth").sum(axis=0)
    two = mul(orth_factor(mul(z_two, z_two.T)), z_two)

    one_own = lax.dynamic_slice_in_dim(one, row * size_one, size_one, 1)
    two_own = lax.dynamic_slice_in_dim(two, col * size_two, size_two, 1)
    core = mul(two, projected.T)
    grid = projected.reshape(-1, rank_one, length_two)
    spread = jnp.einsum("ai,caj->cij", one_own, grid, precision=exact_mode)
    spread = mul(spread.reshape(-1, length_two), mul(two.T, two_own))
    spread = spread.reshape(-1, size_one * size_two)
    core = lax.all_gather(core, "depth")
    spread = lax.all_gather(spread, "depth")
    spread = spread.reshape(depth, cols, slices, -1).transpose(1, 0, 2, 3).reshape(rank_three, -1)
    z_part = mul(spread, flat)
    z_part = from_everyone(z_part, "cols").sum(axis=0)
    z_three = from_everyone(z_part, "rows").sum(axis=0)
    gram = lax.all_gather(mul(z_three, z_three.T), "depth").sum(axis=0)
    three = mul(orth_factor(gram), z_three)

    core = core.reshape(depth, rank_two, cols, slices, rank_one)
    core = core.transpose(4, 1, 2, 0, 3).reshape(rank_one, rank_two, rank_three)
    return (
        one_own.T * math.sqrt(length_one),
        two_own.T * math.sqrt(length_two),
        three.T * math.sqrt(length_three),
        core,
    )


def solution(mesh):
    in_specs = (
        P(("groups", "rows"), "cols", "depth"),
        P(("groups", "rows"), None),
        P(("groups", "cols"), None),
        P(("groups", "depth"), None),
    )
    out_specs = (
        P(("groups", "rows"), None),
        P(("groups", "cols"), None),
        P(("groups", "depth"), None),
        P("groups", None, None),
    )
    return jax.shard_map(body, mesh=mesh, in_specs=in_specs, out_specs=out_specs, check_vma=False)
```

```python
import math

import jax
import jax.numpy as jnp
from jax import lax
from jax.sharding import PartitionSpec as P

NEWTON = 3
LANES = 128
exact_mode = lax.Precision.HIGHEST


def mul(left, right):
    return jnp.dot(left, right, precision=exact_mode)


def from_everyone(shard, axis):
    peers = lax.axis_size(axis)
    return lax.all_to_all(
        jnp.broadcast_to(shard[None], (peers, *shard.shape)), axis, 0, 0, tiled=True
    )


def alone(operation, shard, *others):
    shard, others = lax.optimization_barrier((shard, others))
    return lax.optimization_barrier((operation(shard), *others))


def orth_factor(gram):
    identity = jnp.eye(gram.shape[0], dtype=jnp.float32)
    ones = jnp.ones_like(gram)
    total = mul(ones, mul(gram * identity, ones)) + 1e-06
    gram = gram / total
    factor = None
    for step in range(NEWTON):
        move = 1.5 * identity - 0.5 * gram
        factor = move if factor is None else mul(factor, move)
        if step + 1 < NEWTON:
            gram = mul(mul(move, gram), move)
    return factor / jnp.sqrt(total)


def halves_side_by_side(block):
    half = block.shape[0] // 2
    return jnp.concatenate([block[:half], block[half:]], axis=1)


def halves_stacked(blocks):
    count, half, width = blocks.shape
    width //= 2
    pairs = jnp.stack([blocks[:, :, :width], blocks[:, :, width:]], axis=1)
    return pairs.reshape(count * 2 * half, width)


def body(tensor, start_one, start_two, start_three):
    size_one, size_two, size_three = tensor.shape
    rank_one = start_one.shape[1]
    rank_two = start_two.shape[1]
    rank_three = start_three.shape[1]
    rows, cols, depth = (lax.axis_size(name) for name in ("rows", "cols", "depth"))
    level = lax.axis_index("depth")
    row_from = lax.axis_index("rows") * size_one
    col_from = lax.axis_index("cols") * size_two
    length_one, length_two, length_three = size_one * rows, size_two * cols, size_three * depth
    owners = cols * depth
    slices = rank_three // owners
    flat = tensor.reshape(size_one * size_two, size_three)

    thinned = lax.dot_general(
        start_three, flat, (((0,), (1,)), ((), ())), precision=exact_mode
    ).reshape(owners, -1, LANES)
    two_packed = halves_side_by_side(start_two)
    part = two_packed.shape[0] // depth
    two_part = lax.dynamic_slice_in_dim(two_packed, level * part, part, 0)
    lines = thinned.shape[1]
    message = jnp.concatenate(
        [thinned, jnp.broadcast_to(two_part[None], (owners, *two_part.shape))], axis=1
    )
    one_packed = halves_side_by_side(start_one)
    got, one_packed, flat, row_from, col_from = alone(
        lambda shard: lax.all_to_all(shard, ("cols", "depth"), 0, 0, tiled=True),
        message, one_packed, flat, row_from, col_from,
    )
    got = got.reshape(cols, depth, *got.shape[1:])
    own = got[:, :, :lines].sum(axis=1).reshape(cols, slices * size_one, size_two)
    own = own.transpose(1, 0, 2).reshape(slices * size_one, length_two)
    two_old = halves_stacked(got[:, :, lines:].reshape(cols, depth * part, 2 * rank_two))

    message = jnp.concatenate([own, one_packed], axis=0)
    got, two_old, flat, row_from, col_from = alone(
        lambda shard: from_everyone(shard, "rows"), message, two_old, flat, row_from, col_from
    )
    whole = [
        got[:, c * size_one : (c + 1) * size_one].reshape(length_one, length_two)
        for c in range(slices)
    ]
    one_old = halves_stacked(got[:, slices * size_one :])

    unfolded = jnp.concatenate([mul(matrix, two_old) for matrix in whole], axis=1)
    core = mul(one_old.T, unfolded)
    z_part = mul(core, unfolded.T)
    z_part = lax.all_gather(z_part, "depth").sum(axis=0)
    z_one, two_old, flat, row_from, col_from, *whole = alone(
        lambda shard: from_everyone(shard, "cols"),
        z_part, two_old, flat, row_from, col_from, *whole,
    )
    z_one = z_one.sum(axis=0)
    one = mul(orth_factor(mul(z_one, z_one.T)), z_one)

    projected = jnp.concatenate([mul(one, matrix) for matrix in whole], axis=0)
    projected, two_old, one, flat, row_from, col_from = alone(
        lambda shard: from_everyone(shard, "cols"),
        projected, two_old, one, flat, row_from, col_from,
    )
    projected = projected.reshape(-1, length_two)
    core = mul(projected, two_old)
    z_part = mul(core.T, projected)
    z_two = lax.all_gather(z_part, "depth").sum(axis=0)
    two = mul(orth_factor(mul(z_two, z_two.T)), z_two)

    one_own = lax.dynamic_slice_in_dim(one, row_from, size_one, 1)
    two_own = lax.dynamic_slice_in_dim(two, col_from, size_two, 1)
    grid = projected.reshape(-1, rank_one, length_two)
    spread = jnp.einsum("ai,caj->cij", one_own, grid, precision=exact_mode)
    spread = mul(spread.reshape(-1, length_two), mul(two.T, two_own))
    spread = spread.reshape(-1, size_one * size_two)
    spread = lax.all_gather(spread, "depth")
    spread = spread.reshape(depth, cols, slices, -1).transpose(1, 0, 2, 3).reshape(rank_three, -1)
    z_part = mul(spread, flat)
    z_part, one_own, two_own, two, projected = alone(
        lambda shard: from_everyone(shard, "cols"), z_part, one_own, two_own, two, projected
    )
    z_part = z_part.sum(axis=0)
    z_three = from_everyone(z_part, "rows").sum(axis=0)
    gram = lax.all_gather(mul(z_three, z_three.T), "depth").sum(axis=0)
    three = mul(orth_factor(gram), z_three)

    core = lax.all_gather(mul(two, projected.T), "depth")
    core = core.reshape(depth, rank_two, cols, slices, rank_one)
    core = core.transpose(4, 1, 2, 0, 3).reshape(rank_one, rank_two, rank_three)
    return (
        one_own.T * math.sqrt(length_one),
        two_own.T * math.sqrt(length_two),
        three.T * math.sqrt(length_three),
        core,
    )


def solution(mesh):
    in_specs = (
        P(("groups", "rows"), "cols", "depth"),
        P(("groups", "rows"), None),
        P(("groups", "cols"), None),
        P(("groups", "depth"), None),
    )
    out_specs = (
        P(("groups", "rows"), None),
        P(("groups", "cols"), None),
        P(("groups", "depth"), None),
        P("groups", None, None),
    )
    return jax.shard_map(body, mesh=mesh, in_specs=in_specs, out_specs=out_specs, check_vma=False)
```

```python
import math

import jax
import jax.numpy as jnp
from jax import lax
from jax.sharding import PartitionSpec as P

NEWTON = 3
LANES = 128
CLASSES = 4
exact_mode = lax.Precision.HIGHEST


def mul(left, right):
    return jnp.dot(left, right, precision=exact_mode)


def from_everyone(shard, axis):
    peers = lax.axis_size(axis)
    return lax.all_to_all(
        jnp.broadcast_to(shard[None], (peers, *shard.shape)), axis, 0, 0, tiled=True
    )


def alone(operation, shard, *others):
    shard, others = lax.optimization_barrier((shard, others))
    return lax.optimization_barrier((operation(shard), *others))


def orth_factor(gram):
    identity = jnp.eye(gram.shape[0], dtype=jnp.float32)
    ones = jnp.ones_like(gram)
    total = mul(ones, mul(gram * identity, ones)) + 1e-06
    gram = gram / total
    factor = None
    for step in range(NEWTON):
        move = 1.5 * identity - 0.5 * gram
        factor = move if factor is None else mul(factor, move)
        if step + 1 < NEWTON:
            gram = mul(mul(move, gram), move)
    return factor / jnp.sqrt(total)


def halves_side_by_side(block):
    half = block.shape[0] // 2
    return jnp.concatenate([block[:half], block[half:]], axis=1)


def halves_stacked(blocks):
    count, half, width = blocks.shape
    width //= 2
    pairs = jnp.stack([blocks[:, :, :width], blocks[:, :, width:]], axis=1)
    return pairs.reshape(count * 2 * half, width)


def body(tensor, start_one, start_two, start_three):
    size_one, size_two, size_three = tensor.shape
    rank_one = start_one.shape[1]
    rank_two = start_two.shape[1]
    rank_three = start_three.shape[1]
    rows, cols, depth = (lax.axis_size(name) for name in ("rows", "cols", "depth"))
    row_from = lax.axis_index("rows") * size_one
    col_from = lax.axis_index("cols") * size_two
    length_one, length_two, length_three = size_one * rows, size_two * cols, size_three * depth
    teams = [list(range(first, first + CLASSES)) for first in range(0, cols, CLASSES)]
    slices = rank_three // (CLASSES * depth)
    flat = tensor.reshape(size_one * size_two, size_three)

    thinned = lax.dot_general(
        start_three, flat, (((0,), (1,)), ((), ())), precision=exact_mode
    ).reshape(1, depth, CLASSES, -1, LANES)
    lines = thinned.shape[3]
    two_packed = halves_side_by_side(start_two)
    thinned = jnp.broadcast_to(
        thinned.transpose(0, 2, 1, 3, 4), (len(teams), CLASSES, depth, lines, LANES)
    ).reshape(cols * depth, lines, LANES)
    message = jnp.concatenate(
        [thinned, jnp.broadcast_to(two_packed[None], (cols * depth, *two_packed.shape))], axis=1
    )
    one_packed = halves_side_by_side(start_one)
    got, one_packed, flat, row_from, col_from = alone(
        lambda shard: lax.all_to_all(shard, ("cols", "depth"), 0, 0, tiled=True),
        message, one_packed, flat, row_from, col_from,
    )
    got = got.reshape(cols, depth, *got.shape[1:])
    own = got[:, :, :lines].sum(axis=1).reshape(cols, slices * size_one, size_two)
    own = own.transpose(1, 0, 2).reshape(slices * size_one, length_two)
    two_old = halves_stacked(got[:, 0, lines:])

    got, two_old, flat, row_from, col_from = alone(
        lambda shard: lax.all_gather(shard, "rows"),
        jnp.concatenate([own, one_packed], axis=0), two_old, flat, row_from, col_from,
    )
    whole = [
        got[:, c * size_one : (c + 1) * size_one].reshape(length_one, length_two)
        for c in range(slices)
    ]
    one_old = halves_stacked(got[:, slices * size_one :])

    unfolded = jnp.concatenate([mul(matrix, two_old) for matrix in whole], axis=1)
    core = mul(one_old.T, unfolded)
    z_part = mul(core, unfolded.T)
    z_part = lax.all_gather(z_part, "depth").sum(axis=0)
    z_one = lax.all_gather(z_part, "cols", axis_index_groups=teams).sum(axis=0)
    one = mul(orth_factor(mul(z_one, z_one.T)), z_one)

    projected = jnp.concatenate([mul(one, matrix) for matrix in whole], axis=0)
    projected = lax.all_gather(projected, "cols", axis_index_groups=teams)
    projected = projected.reshape(-1, length_two)
    core = mul(projected, two_old)
    z_part = mul(core.T, projected)
    z_two = lax.all_gather(z_part, "depth").sum(axis=0)
    two = mul(orth_factor(mul(z_two, z_two.T)), z_two)

    one_own = lax.dynamic_slice_in_dim(one, row_from, size_one, 1)
    two_own = lax.dynamic_slice_in_dim(two, col_from, size_two, 1)
    grid = projected.reshape(-1, rank_one, length_two)
    spread = jnp.einsum("ai,caj->cij", one_own, grid, precision=exact_mode)
    spread = mul(spread.reshape(-1, length_two), mul(two.T, two_own))
    spread = spread.reshape(-1, size_one * size_two)
    spread = lax.all_gather(spread, "depth", axis=0, tiled=True)
    z_part = mul(spread, flat)
    z_part, one_own, two_own, two, projected = alone(
        lambda shard: from_everyone(shard, "cols"), z_part, one_own, two_own, two, projected
    )
    z_part = z_part.sum(axis=0)
    z_three = from_everyone(z_part, "rows").sum(axis=0)
    gram = lax.all_gather(mul(z_three, z_three.T), "depth").sum(axis=0)
    three = mul(orth_factor(gram), z_three)

    core = lax.all_gather(mul(two, projected.T), "depth")
    core = core.reshape(depth, rank_two, -1, rank_one)
    core = core.transpose(3, 1, 0, 2).reshape(rank_one, rank_two, rank_three)
    return (
        one_own.T * math.sqrt(length_one),
        two_own.T * math.sqrt(length_two),
        three.T * math.sqrt(length_three),
        core,
    )


def solution(mesh):
    in_specs = (
        P(("groups", "rows"), "cols", "depth"),
        P(("groups", "rows"), None),
        P(("groups", "cols"), None),
        P(("groups", "depth"), None),
    )
    out_specs = (
        P(("groups", "rows"), None),
        P(("groups", "cols"), None),
        P(("groups", "depth"), None),
        P("groups", None, None),
    )
    return jax.shard_map(body, mesh=mesh, in_specs=in_specs, out_specs=out_specs, check_vma=False)
```

```python
import functools
import math

import jax
import jax.numpy as jnp
from jax import lax
from jax.experimental import pallas as pl
from jax.experimental.pallas import tpu as pltpu
from jax.sharding import PartitionSpec as P

NEWTON = 3
LANES = 128
CLASSES = 4
KERNEL_BYTES = 8 * 2**20
exact_mode = lax.Precision.HIGHEST


def mul(left, right):
    return jnp.dot(left, right, precision=exact_mode)


def from_everyone(shard, axis):
    peers = lax.axis_size(axis)
    return lax.all_to_all(
        jnp.broadcast_to(shard[None], (peers, *shard.shape)), axis, 0, 0, tiled=True
    )


def alone(operation, shard, *others):
    shard, others = lax.optimization_barrier((shard, others))
    return lax.optimization_barrier((operation(shard), *others))


def mul_nt(left, right):
    return lax.dot_general(left, right, (((1,), (1,)), ((), ())), precision=exact_mode)


def mul_tn(left, right):
    return lax.dot_general(left, right, (((0,), (0,)), ((), ())), precision=exact_mode)


def orth_factor(gram):
    down = lax.broadcasted_iota(jnp.int32, gram.shape, 0)
    across = lax.broadcasted_iota(jnp.int32, gram.shape, 1)
    identity = (down == across).astype(jnp.float32)
    total = jnp.sum(gram * identity, keepdims=True) + 1e-06
    gram = gram / total
    factor = None
    for step in range(NEWTON):
        move = 1.5 * identity - 0.5 * gram
        factor = move if factor is None else mul(factor, move)
        if step + 1 < NEWTON:
            gram = mul(mul(move, gram), move)
    return factor / jnp.sqrt(total)


def kernel_call(kernel, shapes, *operands):
    one = not isinstance(shapes[0], tuple)
    whole = pl.BlockSpec(memory_space=pltpu.VMEM)
    outs = [jax.ShapeDtypeStruct(shape, jnp.float32) for shape in ([shapes] if one else shapes)]
    return pl.pallas_call(
        kernel,
        out_shape=outs[0] if one else outs,
        in_specs=[whole] * len(operands),
        out_specs=whole if one else [whole] * len(outs),
        compiler_params=pltpu.CompilerParams(vmem_limit_bytes=KERNEL_BYTES),
    )(*operands)


def first_mode(size_one, slices, got, two_old, z_part):
    packed = got[:, slices * size_one :, :]
    width = packed.shape[2] // 2
    one_old = jnp.stack([packed[:, :, :width], packed[:, :, width:]], axis=1)
    one_old = one_old.reshape(-1, width)
    two = two_old[...]
    total = None
    for c in range(slices):
        matrix = got[:, c * size_one : (c + 1) * size_one, :].reshape(-1, two.shape[0])
        unfolded = mul(matrix, two)
        term = mul_nt(mul_tn(one_old, unfolded), unfolded)
        total = term if total is None else total + term
    z_part[...] = total


def to_second(size_one, slices, z_parts, got, one, projected):
    z = jnp.sum(z_parts[...], axis=0)
    new = mul(orth_factor(mul_nt(z, z)), z)
    one[...] = new
    rank = new.shape[0]
    for c in range(slices):
        matrix = got[:, c * size_one : (c + 1) * size_one, :].reshape(new.shape[1], -1)
        projected[c * rank : (c + 1) * rank, :] = mul(new, matrix)


def second_mode(projected, two_old, z_part):
    z_part[...] = mul_tn(mul(projected[...], two_old[...]), projected[...])


def to_third(z_parts, projected, one, one_pick, two_pick, two, one_own, two_own, spread):
    z = jnp.sum(z_parts[...], axis=0)
    new = mul(orth_factor(mul_nt(z, z)), z)
    two[...] = new
    first = mul_nt(one_pick[...], one[...])
    second = mul_nt(two_pick[...], new)
    one_own[...] = first * math.sqrt(one.shape[1])
    two_own[...] = second * math.sqrt(new.shape[1])
    joined = mul(second, new)
    rank = first.shape[1]
    for c in range(projected.shape[0] // rank):
        grid = mul(first, projected[c * rank : (c + 1) * rank, :])
        spread[c * first.shape[0] : (c + 1) * first.shape[0], :] = mul_nt(grid, joined)


def last_orth(scale, grams, z, three):
    factor = orth_factor(jnp.sum(grams[...], axis=0))
    three[...] = mul_tn(z[...], factor) * scale


def own_rows(axis, size, length):
    down = lax.broadcasted_iota(jnp.int32, (size, length), 0)
    across = lax.broadcasted_iota(jnp.int32, (size, length), 1)
    return (across == down + lax.axis_index(axis) * size).astype(jnp.float32)


def halves_side_by_side(block):
    half = block.shape[0] // 2
    return jnp.concatenate([block[:half], block[half:]], axis=1)


def halves_stacked(blocks):
    count, half, width = blocks.shape
    width //= 2
    pairs = jnp.stack([blocks[:, :, :width], blocks[:, :, width:]], axis=1)
    return pairs.reshape(count * 2 * half, width)


def body(tensor, start_one, start_two, start_three):
    size_one, size_two, size_three = tensor.shape
    rank_one = start_one.shape[1]
    rank_two = start_two.shape[1]
    rank_three = start_three.shape[1]
    rows, cols, depth = (lax.axis_size(name) for name in ("rows", "cols", "depth"))
    length_one, length_two, length_three = size_one * rows, size_two * cols, size_three * depth
    one_pick = own_rows("rows", size_one, length_one)
    two_pick = own_rows("cols", size_two, length_two)
    teams = [list(range(first, first + CLASSES)) for first in range(0, cols, CLASSES)]
    half_team = CLASSES // 2
    near = [
        list(range(first * depth, (first + half_team) * depth))
        for first in range(0, cols, half_team)
    ]
    far = [
        [first + at, first + half_team + at]
        for first in range(0, cols, CLASSES)
        for at in range(half_team)
    ]
    slices = rank_three // (CLASSES * depth)
    flat = tensor.reshape(size_one * size_two, size_three)

    thinned = lax.dot_general(
        start_three, flat, (((0,), (1,)), ((), ())), precision=exact_mode
    ).reshape(1, depth, CLASSES, -1, LANES)
    lines = thinned.shape[3]
    two_packed = halves_side_by_side(start_two)
    thinned = jnp.broadcast_to(
        thinned.transpose(0, 2, 1, 3, 4), (len(teams), CLASSES, depth, lines, LANES)
    ).reshape(cols * depth, lines, LANES)
    message = jnp.concatenate(
        [thinned, jnp.broadcast_to(two_packed[None], (cols * depth, *two_packed.shape))], axis=1
    )
    one_packed = halves_side_by_side(start_one)
    got, one_packed, flat, one_pick, two_pick = alone(
        lambda shard: lax.all_to_all(shard, ("cols", "depth"), 0, 0, tiled=True),
        message, one_packed, flat, one_pick, two_pick,
    )
    got = got.reshape(cols, depth, *got.shape[1:])
    own = got[:, :, :lines].sum(axis=1).reshape(cols, slices * size_one, size_two)
    own = own.transpose(1, 0, 2).reshape(slices * size_one, length_two)
    two_old = halves_stacked(got[:, 0, lines:])

    got = lax.all_gather(jnp.concatenate([own, one_packed], axis=0), "rows")

    cut = (size_one, slices)
    z_part = kernel_call(
        functools.partial(first_mode, *cut), (rank_one, length_one), got, two_old
    )
    z_part = lax.all_gather(z_part, ("cols", "depth"), axis_index_groups=near).sum(axis=0)
    z_parts = lax.all_gather(z_part, "cols", axis_index_groups=far)

    one, projected = kernel_call(
        functools.partial(to_second, *cut),
        ((rank_one, length_one), (slices * rank_one, length_two)),
        z_parts,
        got,
    )
    projected = lax.all_gather(projected, "cols", axis_index_groups=teams)
    projected = projected.reshape(-1, length_two)
    z_part = kernel_call(second_mode, (rank_two, length_two), projected, two_old)
    z_parts = lax.all_gather(z_part, "depth")

    half = projected.shape[0] // rank_one
    two, one_own, two_own, spread = kernel_call(
        to_third,
        (
            (rank_two, length_two),
            (size_one, rank_one),
            (size_two, rank_two),
            (half * size_one, size_two),
        ),
        z_parts,
        projected,
        one,
        one_pick,
        two_pick,
    )
    spread = lax.all_gather(spread.reshape(half, -1), "depth", axis=0, tiled=True)
    z_part = mul(spread, flat)
    z_part, two, projected, one_own, two_own = alone(
        lambda shard: from_everyone(shard, "cols"), z_part, two, projected, one_own, two_own
    )
    z_part = z_part.sum(axis=0)
    z_three = from_everyone(z_part, "rows").sum(axis=0)
    grams = lax.all_gather(mul(z_three, z_three.T), "depth")
    three = kernel_call(
        functools.partial(last_orth, math.sqrt(length_three)),
        (size_three, rank_three),
        grams,
        z_three,
    )

    core = lax.all_gather(mul(two, projected.T), "depth")
    core = core.reshape(depth, rank_two, -1, rank_one)
    core = core.transpose(3, 1, 0, 2).reshape(rank_one, rank_two, rank_three)
    return one_own, two_own, three, core


def solution(mesh):
    in_specs = (
        P(("groups", "rows"), "cols", "depth"),
        P(("groups", "rows"), None),
        P(("groups", "cols"), None),
        P(("groups", "depth"), None),
    )
    out_specs = (
        P(("groups", "rows"), None),
        P(("groups", "cols"), None),
        P(("groups", "depth"), None),
        P("groups", None, None),
    )
    return jax.shard_map(body, mesh=mesh, in_specs=in_specs, out_specs=out_specs, check_vma=False)
```

```python
import functools
import math

import jax
import jax.numpy as jnp
from jax import lax
from jax.experimental import pallas as pl
from jax.experimental.pallas import tpu as pltpu
from jax.sharding import PartitionSpec as P

NEWTON = 3
LANES = 128
CLASSES = 4
KERNEL_BYTES = 8 * 2**20
exact_mode = lax.Precision.HIGHEST


def mul(left, right):
    return jnp.dot(left, right, precision=exact_mode)


def from_everyone(shard, axis):
    peers = lax.axis_size(axis)
    return lax.all_to_all(
        jnp.broadcast_to(shard[None], (peers, *shard.shape)), axis, 0, 0, tiled=True
    )


def alone(operation, shard, *others):
    shard, others = lax.optimization_barrier((shard, others))
    return lax.optimization_barrier((operation(shard), *others))


def mul_nt(left, right):
    return lax.dot_general(left, right, (((1,), (1,)), ((), ())), precision=exact_mode)


def mul_tn(left, right):
    return lax.dot_general(left, right, (((0,), (0,)), ((), ())), precision=exact_mode)


def orth_factor(gram):
    down = lax.broadcasted_iota(jnp.int32, gram.shape, 0)
    across = lax.broadcasted_iota(jnp.int32, gram.shape, 1)
    identity = (down == across).astype(jnp.float32)
    total = jnp.sum(gram * identity, keepdims=True) + 1e-06
    gram = gram / total
    factor = None
    for step in range(NEWTON):
        move = 1.5 * identity - 0.5 * gram
        factor = move if factor is None else mul(factor, move)
        if step + 1 < NEWTON:
            gram = mul(mul(move, gram), move)
    return factor / jnp.sqrt(total)


def kernel_call(kernel, shapes, *operands):
    one = not isinstance(shapes[0], tuple)
    whole = pl.BlockSpec(memory_space=pltpu.VMEM)
    outs = [jax.ShapeDtypeStruct(shape, jnp.float32) for shape in ([shapes] if one else shapes)]
    return pl.pallas_call(
        kernel,
        out_shape=outs[0] if one else outs,
        in_specs=[whole] * len(operands),
        out_specs=whole if one else [whole] * len(outs),
        compiler_params=pltpu.CompilerParams(vmem_limit_bytes=KERNEL_BYTES),
    )(*operands)


def class_matrices(got, size_one, slices):
    return [
        got[:, c * size_one : (c + 1) * size_one, :].reshape(-1, got.shape[2])
        for c in range(slices)
    ]


def first_mode(size_one, slices, got, two_old, z_part):
    packed = got[:, slices * size_one :, :]
    width = packed.shape[2] // 2
    one_old = jnp.stack([packed[:, :, :width], packed[:, :, width:]], axis=1)
    one_old = one_old.reshape(-1, width)
    two = two_old[...]
    none = jnp.zeros_like(two)
    twice = jnp.concatenate(
        [jnp.concatenate([two, none], axis=1), jnp.concatenate([none, two], axis=1)], axis=0
    )
    whole = class_matrices(got, size_one, slices)
    pairs = [jnp.concatenate(whole[c : c + 2], axis=1) for c in range(0, slices, 2)]
    unfolded = jnp.concatenate([mul(pair, twice) for pair in pairs], axis=1)
    z_part[...] = mul_nt(mul(one_old.T, unfolded), unfolded)


def to_second(size_one, slices, z_parts, got, one, projected):
    z = jnp.sum(z_parts[...], axis=0)
    new = mul(orth_factor(mul_nt(z, z)), z)
    one[...] = new
    rank = new.shape[0]
    width = got.shape[2]
    wide = mul(new, jnp.concatenate(class_matrices(got, size_one, slices), axis=1))
    for c in range(slices):
        projected[c * rank : (c + 1) * rank, :] = wide[:, c * width : (c + 1) * width]


def second_mode(projected, two_old, z_part):
    z_part[...] = mul(mul_nt(two_old[...].T, projected[...]), projected[...])


def to_third(z_parts, projected, one, two, one_own, two_own, spread):
    z = jnp.sum(z_parts[...], axis=0)
    new = mul(orth_factor(mul_nt(z, z)), z)
    two[...] = new
    rank, length_one = one.shape
    length_two = new.shape[1]
    size_one, size_two = one_own.shape[0], two_own.shape[0]
    first = mul_nt(own_rows("rows", size_one, length_one), one[...])
    second = mul_nt(own_rows("cols", size_two, length_two), new)
    one_own[...] = first * math.sqrt(length_one)
    two_own[...] = second * math.sqrt(length_two)
    held = projected.shape[0] // rank
    wide = jnp.concatenate(
        [projected[c * rank : (c + 1) * rank, :] for c in range(held)], axis=1
    )
    wide = mul(first, wide)
    tall = jnp.concatenate(
        [wide[:, c * length_two : (c + 1) * length_two] for c in range(held)], axis=0
    )
    spread[...] = mul_nt(tall, mul(second, new))


def last_orth(scale, grams, z, three):
    three[...] = mul(orth_factor(jnp.sum(grams[...], axis=0)), z[...]) * scale


def own_rows(axis, size, length):
    down = lax.broadcasted_iota(jnp.int32, (size, length), 0)
    across = lax.broadcasted_iota(jnp.int32, (size, length), 1)
    return (across == down + lax.axis_index(axis) * size).astype(jnp.float32)


def halves_side_by_side(block):
    half = block.shape[0] // 2
    return jnp.concatenate([block[:half], block[half:]], axis=1)


def halves_stacked(blocks):
    count, half, width = blocks.shape
    width //= 2
    pairs = jnp.stack([blocks[:, :, :width], blocks[:, :, width:]], axis=1)
    return pairs.reshape(count * 2 * half, width)


def body(tensor, start_one, start_two, start_three):
    size_one, size_two, size_three = tensor.shape
    rank_one = start_one.shape[1]
    rank_two = start_two.shape[1]
    rank_three = start_three.shape[1]
    rows, cols, depth = (lax.axis_size(name) for name in ("rows", "cols", "depth"))
    length_one, length_two, length_three = size_one * rows, size_two * cols, size_three * depth
    teams = [list(range(first, first + CLASSES)) for first in range(0, cols, CLASSES)]
    half_team = CLASSES // 2
    near = [
        list(range(first * depth, (first + half_team) * depth))
        for first in range(0, cols, half_team)
    ]
    far = [
        [first + at, first + half_team + at]
        for first in range(0, cols, CLASSES)
        for at in range(half_team)
    ]
    slices = rank_three // (CLASSES * depth)
    flat = tensor.reshape(size_one * size_two, size_three)

    thinned = lax.dot_general(
        start_three, flat, (((0,), (1,)), ((), ())), precision=exact_mode
    ).reshape(1, depth, CLASSES, -1, LANES)
    lines = thinned.shape[3]
    two_packed = halves_side_by_side(start_two)
    thinned = jnp.broadcast_to(
        thinned.transpose(0, 2, 1, 3, 4), (len(teams), CLASSES, depth, lines, LANES)
    ).reshape(cols * depth, lines, LANES)
    message = jnp.concatenate(
        [thinned, jnp.broadcast_to(two_packed[None], (cols * depth, *two_packed.shape))], axis=1
    )
    one_packed = halves_side_by_side(start_one)
    got, one_packed, flat = alone(
        lambda shard: lax.all_to_all(shard, ("cols", "depth"), 0, 0, tiled=True),
        message, one_packed, flat,
    )
    got = got.reshape(cols, depth, *got.shape[1:])
    own = got[:, :, :lines].sum(axis=1).reshape(cols, slices * size_one, size_two)
    own = own.transpose(1, 0, 2).reshape(slices * size_one, length_two)
    two_old = halves_stacked(got[:, 0, lines:])

    got = lax.all_gather(jnp.concatenate([own, one_packed], axis=0), "rows")

    cut = (size_one, slices)
    z_part = kernel_call(
        functools.partial(first_mode, *cut), (rank_one, length_one), got, two_old
    )
    z_part = lax.all_gather(z_part, ("cols", "depth"), axis_index_groups=near).sum(axis=0)
    z_parts = lax.all_gather(z_part, "cols", axis_index_groups=far)

    one, projected = kernel_call(
        functools.partial(to_second, *cut),
        ((rank_one, length_one), (slices * rank_one, length_two)),
        z_parts,
        got,
    )
    projected = lax.all_gather(projected, "cols", axis_index_groups=teams)
    projected = projected.reshape(-1, length_two)
    z_part = kernel_call(second_mode, (rank_two, length_two), projected, two_old)
    z_parts = lax.all_gather(z_part, "depth")

    half = projected.shape[0] // rank_one
    two, one_own, two_own, spread = kernel_call(
        to_third,
        (
            (rank_two, length_two),
            (size_one, rank_one),
            (size_two, rank_two),
            (half * size_one, size_two),
        ),
        z_parts,
        projected,
        one,
    )
    spread = lax.all_gather(spread.reshape(half, -1), "depth", axis=0, tiled=True)
    z_part = mul(spread, flat)
    z_part, two, projected, one_own, two_own = alone(
        lambda shard: from_everyone(shard, "cols"), z_part, two, projected, one_own, two_own
    )
    z_part = z_part.sum(axis=0)
    z_three = from_everyone(z_part, "rows").sum(axis=0)
    grams = lax.all_gather(mul(z_three, z_three.T), "depth")
    three = kernel_call(
        functools.partial(last_orth, math.sqrt(length_three)),
        (rank_three, size_three),
        grams,
        z_three,
    )

    core = lax.all_gather(mul(two, projected.T), "depth")
    core = core.reshape(depth, rank_two, -1, rank_one)
    core = core.transpose(3, 1, 0, 2).reshape(rank_one, rank_two, rank_three)
    return one_own, two_own, three.T, core


def solution(mesh):
    in_specs = (
        P(("groups", "rows"), "cols", "depth"),
        P(("groups", "rows"), None),
        P(("groups", "cols"), None),
        P(("groups", "depth"), None),
    )
    out_specs = (
        P(("groups", "rows"), None),
        P(("groups", "cols"), None),
        P(("groups", "depth"), None),
        P("groups", None, None),
    )
    return jax.shard_map(body, mesh=mesh, in_specs=in_specs, out_specs=out_specs, check_vma=False)
```

```python
import functools
import math

import jax
import jax.numpy as jnp
from jax import lax
from jax.experimental import pallas as pl
from jax.experimental.pallas import tpu as pltpu
from jax.sharding import PartitionSpec as P

NEWTON = 3
LANES = 128
CLASSES = 4
KERNEL_BYTES = 8 * 2**20
exact_mode = lax.Precision.HIGHEST


def mul(left, right):
    return jnp.dot(left, right, precision=exact_mode)


def from_everyone(shard, axis):
    peers = lax.axis_size(axis)
    return lax.all_to_all(
        jnp.broadcast_to(shard[None], (peers, *shard.shape)), axis, 0, 0, tiled=True
    )


def alone(operation, shard, *others):
    shard, others = lax.optimization_barrier((shard, others))
    return lax.optimization_barrier((operation(shard), *others))


def mul_nt(left, right):
    return lax.dot_general(left, right, (((1,), (1,)), ((), ())), precision=exact_mode)


def mul_tn(left, right):
    return lax.dot_general(left, right, (((0,), (0,)), ((), ())), precision=exact_mode)


def orth_factor(gram):
    down = lax.broadcasted_iota(jnp.int32, gram.shape, 0)
    across = lax.broadcasted_iota(jnp.int32, gram.shape, 1)
    identity = (down == across).astype(jnp.float32)
    total = jnp.sum(gram * identity, keepdims=True) + 1e-06
    gram = gram / total
    factor = None
    for step in range(NEWTON):
        move = 1.5 * identity - 0.5 * gram
        factor = move if factor is None else mul(factor, move)
        if step + 1 < NEWTON:
            gram = mul(mul(move, gram), move)
    return factor / jnp.sqrt(total)


def kernel_call(kernel, shapes, *operands):
    one = not isinstance(shapes[0], tuple)
    whole = pl.BlockSpec(memory_space=pltpu.VMEM)
    outs = [jax.ShapeDtypeStruct(shape, jnp.float32) for shape in ([shapes] if one else shapes)]
    return pl.pallas_call(
        kernel,
        out_shape=outs[0] if one else outs,
        in_specs=[whole] * len(operands),
        out_specs=whole if one else [whole] * len(outs),
        compiler_params=pltpu.CompilerParams(vmem_limit_bytes=KERNEL_BYTES),
    )(*operands)


def class_matrices(got, size_one, slices):
    return [
        got[:, c * size_one : (c + 1) * size_one, :].reshape(-1, got.shape[2])
        for c in range(slices)
    ]


def first_mode(size_one, slices, got, two_old, z_part):
    packed = got[:, slices * size_one :, :]
    width = packed.shape[2] // 2
    one_old = jnp.stack([packed[:, :, :width], packed[:, :, width:]], axis=1)
    one_old = one_old.reshape(-1, width)
    two = two_old[...]
    none = jnp.zeros_like(two)
    twice = jnp.concatenate(
        [jnp.concatenate([two, none], axis=1), jnp.concatenate([none, two], axis=1)], axis=0
    )
    whole = class_matrices(got, size_one, slices)
    pairs = [jnp.concatenate(whole[c : c + 2], axis=1) for c in range(0, slices, 2)]
    unfolded = jnp.concatenate([mul(pair, twice) for pair in pairs], axis=1)
    z_part[...] = mul_nt(mul(one_old.T, unfolded), unfolded)


def to_second(size_one, slices, z_parts, got, one, projected):
    z = jnp.sum(z_parts[...], axis=0)
    new = mul(orth_factor(mul_nt(z, z)), z)
    one[...] = new
    rank = new.shape[0]
    width = got.shape[2]
    wide = mul(new, jnp.concatenate(class_matrices(got, size_one, slices), axis=1))
    for c in range(slices):
        projected[c * rank : (c + 1) * rank, :] = wide[:, c * width : (c + 1) * width]


def second_mode(projected, two_old, z_part):
    z_part[...] = mul(mul_nt(two_old[...].T, projected[...]), projected[...])


def to_third(z_parts, projected, one, two, one_own, two_own, spread):
    z = jnp.sum(z_parts[...], axis=0)
    new = mul(orth_factor(mul_nt(z, z)), z)
    two[...] = new
    rank, length_one = one.shape
    length_two = new.shape[1]
    size_one, size_two = one_own.shape[0], two_own.shape[0]
    first = mul_nt(own_rows("rows", size_one, length_one), one[...])
    second = mul_nt(own_rows("cols", size_two, length_two), new)
    one_own[...] = first
    two_own[...] = second
    held = projected.shape[0] // rank
    wide = jnp.concatenate(
        [projected[c * rank : (c + 1) * rank, :] for c in range(held)], axis=1
    )
    wide = mul(first, wide)
    tall = jnp.concatenate(
        [wide[:, c * length_two : (c + 1) * length_two] for c in range(held)], axis=0
    )
    spread[...] = mul_nt(tall, mul(second, new))


def last_orth(scale, parts, three):
    shares = parts.shape[0]
    whole = [
        jnp.concatenate([parts[share, level] for share in range(shares)], axis=0)
        for level in range(parts.shape[1])
    ]
    gram = functools.reduce(jnp.add, [mul_nt(z, z) for z in whole])
    own = whole[0]
    for level in range(1, len(whole)):
        own = jnp.where(lax.axis_index("depth") == level, whole[level], own)
    three[...] = mul(orth_factor(gram), own) * scale


def own_rows(axis, size, length):
    down = lax.broadcasted_iota(jnp.int32, (size, length), 0)
    across = lax.broadcasted_iota(jnp.int32, (size, length), 1)
    return (across == down + lax.axis_index(axis) * size).astype(jnp.float32)


def halves_side_by_side(block):
    half = block.shape[0] // 2
    return jnp.concatenate([block[:half], block[half:]], axis=1)


def halves_stacked(blocks):
    count, half, width = blocks.shape
    width //= 2
    pairs = jnp.stack([blocks[:, :, :width], blocks[:, :, width:]], axis=1)
    return pairs.reshape(count * 2 * half, width)


def body(tensor, start_one, start_two, start_three):
    size_one, size_two, size_three = tensor.shape
    rank_one = start_one.shape[1]
    rank_two = start_two.shape[1]
    rank_three = start_three.shape[1]
    rows, cols, depth = (lax.axis_size(name) for name in ("rows", "cols", "depth"))
    length_one, length_two, length_three = size_one * rows, size_two * cols, size_three * depth
    teams = [list(range(first, first + CLASSES)) for first in range(0, cols, CLASSES)]
    half_team = CLASSES // 2
    near = [
        list(range(first * depth, (first + half_team) * depth))
        for first in range(0, cols, half_team)
    ]
    far = [
        [first + at, first + half_team + at]
        for first in range(0, cols, CLASSES)
        for at in range(half_team)
    ]
    slices = rank_three // (CLASSES * depth)
    flat = tensor.reshape(size_one * size_two, size_three)

    thinned = lax.dot_general(
        start_three, flat, (((0,), (1,)), ((), ())), precision=exact_mode
    ).reshape(1, depth, CLASSES, -1, LANES)
    lines = thinned.shape[3]
    two_packed = halves_side_by_side(start_two)
    thinned = jnp.broadcast_to(
        thinned.transpose(0, 2, 1, 3, 4), (len(teams), CLASSES, depth, lines, LANES)
    ).reshape(cols * depth, lines, LANES)
    message = jnp.concatenate(
        [thinned, jnp.broadcast_to(two_packed[None], (cols * depth, *two_packed.shape))], axis=1
    )
    one_packed = halves_side_by_side(start_one)
    got, one_packed, flat = alone(
        lambda shard: lax.all_to_all(shard, ("cols", "depth"), 0, 0, tiled=True),
        message, one_packed, flat,
    )
    got = got.reshape(cols, depth, *got.shape[1:])
    own = got[:, :, :lines].sum(axis=1).reshape(cols, slices * size_one, size_two)
    own = own.transpose(1, 0, 2).reshape(slices * size_one, length_two)
    two_old = halves_stacked(got[:, 0, lines:])

    got = lax.all_gather(jnp.concatenate([own, one_packed], axis=0), "rows")

    cut = (size_one, slices)
    z_part = kernel_call(
        functools.partial(first_mode, *cut), (rank_one, length_one), got, two_old
    )
    z_part = lax.all_gather(z_part, ("cols", "depth"), axis_index_groups=near).sum(axis=0)
    z_parts = lax.all_gather(z_part, "cols", axis_index_groups=far)

    one, projected = kernel_call(
        functools.partial(to_second, *cut),
        ((rank_one, length_one), (slices * rank_one, length_two)),
        z_parts,
        got,
    )
    projected = lax.all_gather(projected, "cols", axis_index_groups=teams)
    projected = projected.reshape(-1, length_two)
    z_part = kernel_call(second_mode, (rank_two, length_two), projected, two_old)
    z_parts = lax.all_gather(z_part, "depth")

    half = projected.shape[0] // rank_one
    two, one_own, two_own, spread = kernel_call(
        to_third,
        (
            (rank_two, length_two),
            (size_one, rank_one),
            (size_two, rank_two),
            (half * size_one, size_two),
        ),
        z_parts,
        projected,
        one,
    )
    spread = lax.all_gather(spread.reshape(half, -1), "depth", axis=0, tiled=True)
    shares = jnp.broadcast_to(
        mul(spread, flat).reshape(1, half_team, -1, size_three),
        (cols // half_team, half_team, rank_three // half_team, size_three),
    ).reshape(cols, -1, size_three)
    z_part, two, projected, one_own, two_own = alone(
        lambda shard: lax.all_to_all(shard, "cols", 0, 0, tiled=True),
        shares, two, projected, one_own, two_own,
    )
    z_part = from_everyone(z_part.sum(axis=0), "rows").sum(axis=0)
    z_parts = lax.all_gather(z_part, ("cols", "depth"), axis_index_groups=near)
    three = kernel_call(
        functools.partial(last_orth, math.sqrt(length_three)),
        (rank_three, size_three),
        z_parts.reshape(half_team, depth, -1, size_three),
    )

    core = lax.all_gather(mul(two, projected.T), "depth")
    core = core.reshape(depth, rank_two, -1, rank_one)
    core = core.transpose(3, 1, 0, 2).reshape(rank_one, rank_two, rank_three)
    return (
        one_own * math.sqrt(length_one),
        two_own * math.sqrt(length_two),
        three.T,
        core,
    )


def solution(mesh):
    in_specs = (
        P(("groups", "rows"), "cols", "depth"),
        P(("groups", "rows"), None),
        P(("groups", "cols"), None),
        P(("groups", "depth"), None),
    )
    out_specs = (
        P(("groups", "rows"), None),
        P(("groups", "cols"), None),
        P(("groups", "depth"), None),
        P("groups", None, None),
    )
    return jax.shard_map(body, mesh=mesh, in_specs=in_specs, out_specs=out_specs, check_vma=False)
```

```python
import functools
import math

import jax
import jax.numpy as jnp
from jax import lax
from jax.experimental import pallas as pl
from jax.experimental.pallas import tpu as pltpu
from jax.sharding import PartitionSpec as P

NEWTON = 3
LANES = 128
CLASSES = 4
EVERYWHERE = ("rows", "cols", "depth")
KERNEL_BYTES = 8 * 2**20
exact_mode = lax.Precision.HIGHEST


def mul(left, right):
    return jnp.dot(left, right, precision=exact_mode)


def from_everyone(shard, axis):
    peers = lax.axis_size(axis)
    return lax.all_to_all(
        jnp.broadcast_to(shard[None], (peers, *shard.shape)), axis, 0, 0, tiled=True
    )


def alone(operation, shard, *others):
    shard, others = lax.optimization_barrier((shard, others))
    return lax.optimization_barrier((operation(shard), *others))


def mul_nt(left, right):
    return lax.dot_general(left, right, (((1,), (1,)), ((), ())), precision=exact_mode)


def mul_tn(left, right):
    return lax.dot_general(left, right, (((0,), (0,)), ((), ())), precision=exact_mode)


def orth_factor(gram):
    down = lax.broadcasted_iota(jnp.int32, gram.shape, 0)
    across = lax.broadcasted_iota(jnp.int32, gram.shape, 1)
    identity = (down == across).astype(jnp.float32)
    total = jnp.sum(gram * identity, keepdims=True) + 1e-06
    gram = gram / total
    factor = None
    for step in range(NEWTON):
        move = 1.5 * identity - 0.5 * gram
        factor = move if factor is None else mul(factor, move)
        if step + 1 < NEWTON:
            gram = mul(mul(move, gram), move)
    return factor / jnp.sqrt(total)


def kernel_call(kernel, shapes, *operands):
    one = not isinstance(shapes[0], tuple)
    whole = pl.BlockSpec(memory_space=pltpu.VMEM)
    outs = [jax.ShapeDtypeStruct(shape, jnp.float32) for shape in ([shapes] if one else shapes)]
    return pl.pallas_call(
        kernel,
        out_shape=outs[0] if one else outs,
        in_specs=[whole] * len(operands),
        out_specs=whole if one else [whole] * len(outs),
        compiler_params=pltpu.CompilerParams(vmem_limit_bytes=KERNEL_BYTES),
    )(*operands)


def class_matrices(got, size_one, slices):
    return [
        got[:, c * size_one : (c + 1) * size_one, :].reshape(-1, got.shape[2])
        for c in range(slices)
    ]


def first_mode(size_one, slices, got, two_old, z_part):
    packed = got[:, slices * size_one :, :]
    width = packed.shape[2] // 2
    one_old = jnp.stack([packed[:, :, :width], packed[:, :, width:]], axis=1)
    one_old = one_old.reshape(-1, width)
    two = two_old[...]
    none = jnp.zeros_like(two)
    twice = jnp.concatenate(
        [jnp.concatenate([two, none], axis=1), jnp.concatenate([none, two], axis=1)], axis=0
    )
    whole = class_matrices(got, size_one, slices)
    pairs = [jnp.concatenate(whole[c : c + 2], axis=1) for c in range(0, slices, 2)]
    unfolded = jnp.concatenate([mul(pair, twice) for pair in pairs], axis=1)
    z_part[...] = mul_nt(mul(one_old.T, unfolded), unfolded)


def to_second(size_one, slices, z_parts, got, one, projected):
    z = jnp.sum(z_parts[...], axis=0)
    new = mul(orth_factor(mul_nt(z, z)), z)
    one[...] = new
    rank = new.shape[0]
    width = got.shape[2]
    wide = mul(new, jnp.concatenate(class_matrices(got, size_one, slices), axis=1))
    for c in range(slices):
        projected[c * rank : (c + 1) * rank, :] = wide[:, c * width : (c + 1) * width]


def second_mode(projected, two_old, z_part):
    z_part[...] = mul(mul_nt(two_old[...].T, projected[...]), projected[...])


def to_third(z_parts, projected, one, two, one_own, two_own, spread):
    z = jnp.sum(z_parts[...], axis=0)
    new = mul(orth_factor(mul_nt(z, z)), z)
    two[...] = new
    rank, length_one = one.shape
    length_two = new.shape[1]
    size_one, size_two = one_own.shape[0], two_own.shape[0]
    first = mul_nt(own_rows("rows", size_one, length_one), one[...])
    second = mul_nt(own_rows("cols", size_two, length_two), new)
    one_own[...] = first
    two_own[...] = second
    held = projected.shape[0] // rank
    wide = jnp.concatenate(
        [projected[c * rank : (c + 1) * rank, :] for c in range(held)], axis=1
    )
    wide = mul(first, wide)
    tall = jnp.concatenate(
        [wide[:, c * length_two : (c + 1) * length_two] for c in range(held)], axis=0
    )
    spread[...] = mul_nt(tall, mul(second, new))


def last_orth(scale, parts, three):
    shares = parts.shape[0]
    whole = [
        jnp.concatenate([parts[share, level] for share in range(shares)], axis=0)
        for level in range(parts.shape[1])
    ]
    gram = functools.reduce(jnp.add, [mul_nt(z, z) for z in whole])
    own = whole[0]
    for level in range(1, len(whole)):
        own = jnp.where(lax.axis_index("depth") == level, whole[level], own)
    three[...] = mul(orth_factor(gram), own) * scale


def own_rows(axis, size, length):
    down = lax.broadcasted_iota(jnp.int32, (size, length), 0)
    across = lax.broadcasted_iota(jnp.int32, (size, length), 1)
    return (across == down + lax.axis_index(axis) * size).astype(jnp.float32)


def halves_side_by_side(block):
    half = block.shape[0] // 2
    return jnp.concatenate([block[:half], block[half:]], axis=1)


def halves_stacked(blocks):
    count, half, width = blocks.shape
    width //= 2
    pairs = jnp.stack([blocks[:, :, :width], blocks[:, :, width:]], axis=1)
    return pairs.reshape(count * 2 * half, width)


def body(tensor, start_one, start_two, start_three):
    size_one, size_two, size_three = tensor.shape
    rank_one = start_one.shape[1]
    rank_two = start_two.shape[1]
    rank_three = start_three.shape[1]
    rows, cols, depth = (lax.axis_size(name) for name in ("rows", "cols", "depth"))
    length_one, length_two, length_three = size_one * rows, size_two * cols, size_three * depth
    half_team = CLASSES // 2

    def core_of(half, row, col):
        return (half + row + col) % depth

    blocks = [
        [(row * cols + col) * depth + core_of(half, row, col) for col in range(cols) for half in range(depth)]
        for row in range(rows)
    ]
    chips = [order[at : at + depth] for order in blocks for at in range(0, cols * depth, depth)]
    lines_of_chips = [
        [row * depth + core_of(half, row, 0) for row in range(rows)] for half in range(depth)
    ]
    teams = [
        [col * depth + core_of(half, 0, col) for col in range(first, first + CLASSES)]
        for first in range(0, cols, CLASSES)
        for half in range(depth)
    ]
    near = [
        list(range(first * depth, (first + half_team) * depth))
        for first in range(0, cols, half_team)
    ]
    far = [
        [first + at, first + half_team + at]
        for first in range(0, cols, CLASSES)
        for at in range(half_team)
    ]
    slices = rank_three // (CLASSES * depth)
    flat = tensor.reshape(size_one * size_two, size_three)

    thinned = lax.dot_general(
        start_three, flat, (((0,), (1,)), ((), ())), precision=exact_mode
    ).reshape(1, depth, CLASSES, -1, LANES)
    lines = thinned.shape[3]
    two_packed = halves_side_by_side(start_two)
    thinned = jnp.broadcast_to(
        thinned.transpose(0, 2, 1, 3, 4), (cols // CLASSES, CLASSES, depth, lines, LANES)
    ).reshape(cols * depth, lines, LANES)
    message = jnp.concatenate(
        [thinned, jnp.broadcast_to(two_packed[None], (cols * depth, *two_packed.shape))], axis=1
    )
    one_packed = halves_side_by_side(start_one)
    got, one_packed, flat = alone(
        lambda shard: lax.all_to_all(
            shard, EVERYWHERE, 0, 0, tiled=True, axis_index_groups=blocks
        ),
        message, one_packed, flat,
    )
    got = got.reshape(cols, depth, *got.shape[1:])
    own = got[:, :, :lines].sum(axis=1).reshape(cols, slices * size_one, size_two)
    own = own.transpose(1, 0, 2).reshape(slices * size_one, length_two)
    two_old = halves_stacked(got[:, 0, lines:])

    got = lax.all_gather(
        jnp.concatenate([own, one_packed], axis=0),
        ("rows", "depth"),
        axis_index_groups=lines_of_chips,
    )

    cut = (size_one, slices)
    z_part = kernel_call(
        functools.partial(first_mode, *cut), (rank_one, length_one), got, two_old
    )
    z_part = lax.all_gather(z_part, ("cols", "depth"), axis_index_groups=near).sum(axis=0)
    z_parts = lax.all_gather(z_part, "cols", axis_index_groups=far)

    one, projected = kernel_call(
        functools.partial(to_second, *cut),
        ((rank_one, length_one), (slices * rank_one, length_two)),
        z_parts,
        got,
    )
    projected = lax.all_gather(projected, ("cols", "depth"), axis_index_groups=teams)
    projected = projected.reshape(-1, length_two)
    z_part = kernel_call(second_mode, (rank_two, length_two), projected, two_old)
    z_parts = lax.all_gather(z_part, "depth")

    half = projected.shape[0] // rank_one
    two, one_own, two_own, spread = kernel_call(
        to_third,
        (
            (rank_two, length_two),
            (size_one, rank_one),
            (size_two, rank_two),
            (half * size_one, size_two),
        ),
        z_parts,
        projected,
        one,
    )
    spread = lax.all_gather(spread.reshape(half, -1), EVERYWHERE, axis_index_groups=chips)
    spread = spread.reshape(rank_three, -1)
    shares = jnp.broadcast_to(
        mul(spread, flat).reshape(1, half_team, -1, size_three),
        (cols // half_team, half_team, rank_three // half_team, size_three),
    ).reshape(cols, -1, size_three)
    z_part, two, projected, one_own, two_own = alone(
        lambda shard: lax.all_to_all(shard, "cols", 0, 0, tiled=True),
        shares, two, projected, one_own, two_own,
    )
    z_part = from_everyone(z_part.sum(axis=0), "rows").sum(axis=0)
    z_parts = lax.all_gather(z_part, ("cols", "depth"), axis_index_groups=near)
    three = kernel_call(
        functools.partial(last_orth, math.sqrt(length_three)),
        (rank_three, size_three),
        z_parts.reshape(half_team, depth, -1, size_three),
    )

    core = lax.all_gather(
        mul(two, projected.T), EVERYWHERE, axis_index_groups=chips
    )
    core = core.reshape(depth, rank_two, -1, rank_one)
    core = core.transpose(3, 1, 0, 2).reshape(rank_one, rank_two, rank_three)
    return (
        one_own * math.sqrt(length_one),
        two_own * math.sqrt(length_two),
        three.T,
        core,
    )


def solution(mesh):
    in_specs = (
        P(("groups", "rows"), "cols", "depth"),
        P(("groups", "rows"), None),
        P(("groups", "cols"), None),
        P(("groups", "depth"), None),
    )
    out_specs = (
        P(("groups", "rows"), None),
        P(("groups", "cols"), None),
        P(("groups", "depth"), None),
        P("groups", None, None),
    )
    return jax.shard_map(body, mesh=mesh, in_specs=in_specs, out_specs=out_specs, check_vma=False)
```

```python
import functools
import math

import jax
import jax.numpy as jnp
from jax import lax
from jax.experimental import pallas as pl
from jax.experimental.pallas import tpu as pltpu
from jax.sharding import PartitionSpec as P

NEWTON = 3
LANES = 128
CLASSES = 4
EVERYWHERE = ("rows", "cols", "depth")
KERNEL_BYTES = 8 * 2**20
exact_mode = lax.Precision.HIGHEST


def mul(left, right):
    return jnp.dot(left, right, precision=exact_mode)


def from_everyone(shard, axis):
    peers = lax.axis_size(axis)
    return lax.all_to_all(
        jnp.broadcast_to(shard[None], (peers, *shard.shape)), axis, 0, 0, tiled=True
    )


def alone(operation, shard, *others):
    shard, others = lax.optimization_barrier((shard, others))
    return lax.optimization_barrier((operation(shard), *others))


def mul_nt(left, right):
    return lax.dot_general(left, right, (((1,), (1,)), ((), ())), precision=exact_mode)


def head_and_rest(matrix):
    head = matrix.astype(jnp.bfloat16)
    return head, (matrix - head.astype(jnp.float32)).astype(jnp.bfloat16)


def three_products(left, right, contract):
    left_head, left_rest = head_and_rest(left)
    right_head, right_rest = head_and_rest(right)

    def product(one, other):
        return lax.dot_general(
            one, other, (contract, ((), ())), preferred_element_type=jnp.float32
        )

    small = product(left_head, right_rest) + product(left_rest, right_head)
    return product(left_head, right_head) + small


def times(left, right):
    return three_products(left, right, ((1,), (0,)))


def gram_of(z):
    return three_products(z, z, ((1,), (1,)))


def orth_factor(gram):
    down = lax.broadcasted_iota(jnp.int32, gram.shape, 0)
    across = lax.broadcasted_iota(jnp.int32, gram.shape, 1)
    identity = (down == across).astype(jnp.float32)
    total = jnp.sum(gram * identity, keepdims=True) + 1e-06
    gram = gram / total
    factor = None
    for step in range(NEWTON):
        move = 1.5 * identity - 0.5 * gram
        factor = move if factor is None else times(factor, move)
        if step + 1 < NEWTON:
            gram = times(times(move, gram), move)
    return factor / jnp.sqrt(total)


def kernel_call(kernel, shapes, *operands):
    one = not isinstance(shapes[0], tuple)
    whole = pl.BlockSpec(memory_space=pltpu.VMEM)
    outs = [jax.ShapeDtypeStruct(shape, jnp.float32) for shape in ([shapes] if one else shapes)]
    return pl.pallas_call(
        kernel,
        out_shape=outs[0] if one else outs,
        in_specs=[whole] * len(operands),
        out_specs=whole if one else [whole] * len(outs),
        compiler_params=pltpu.CompilerParams(vmem_limit_bytes=KERNEL_BYTES),
    )(*operands)


def class_matrices(got, size_one, slices):
    return [
        got[:, c * size_one : (c + 1) * size_one, :].reshape(-1, got.shape[2])
        for c in range(slices)
    ]


def first_mode(size_one, slices, got, two_old, z_part):
    packed = got[:, slices * size_one :, :]
    width = packed.shape[2] // 2
    one_old = jnp.stack([packed[:, :, :width], packed[:, :, width:]], axis=1)
    one_old = one_old.reshape(-1, width)
    two = two_old[...]
    none = jnp.zeros_like(two)
    twice = jnp.concatenate(
        [jnp.concatenate([two, none], axis=1), jnp.concatenate([none, two], axis=1)], axis=0
    )
    whole = class_matrices(got, size_one, slices)
    pairs = [jnp.concatenate(whole[c : c + 2], axis=1) for c in range(0, slices, 2)]
    unfolded = jnp.concatenate([mul(pair, twice) for pair in pairs], axis=1)
    z_part[...] = mul_nt(mul(one_old.T, unfolded), unfolded)


def to_second(size_one, slices, z_parts, got, one, projected):
    z = jnp.sum(z_parts[...], axis=0)
    new = times(orth_factor(gram_of(z)), z)
    one[...] = new
    rank = new.shape[0]
    width = got.shape[2]
    wide = mul(new, jnp.concatenate(class_matrices(got, size_one, slices), axis=1))
    for c in range(slices):
        projected[c * rank : (c + 1) * rank, :] = wide[:, c * width : (c + 1) * width]


def second_mode(projected, two_old, z_part):
    z_part[...] = mul(mul_nt(two_old[...].T, projected[...]), projected[...])


def to_third(z_parts, projected, one, two, one_own, two_own, spread):
    z = jnp.sum(z_parts[...], axis=0)
    new = times(orth_factor(gram_of(z)), z)
    two[...] = new
    rank, length_one = one.shape
    length_two = new.shape[1]
    size_one, size_two = one_own.shape[0], two_own.shape[0]
    first = mul_nt(own_rows("rows", size_one, length_one), one[...])
    second = mul_nt(own_rows("cols", size_two, length_two), new)
    one_own[...] = first
    two_own[...] = second
    held = projected.shape[0] // rank
    wide = jnp.concatenate(
        [projected[c * rank : (c + 1) * rank, :] for c in range(held)], axis=1
    )
    wide = mul(first, wide)
    tall = jnp.concatenate(
        [wide[:, c * length_two : (c + 1) * length_two] for c in range(held)], axis=0
    )
    spread[...] = mul_nt(tall, mul(second, new))


def last_orth(scale, parts, three):
    shares = parts.shape[0]
    whole = [
        jnp.concatenate([parts[share, level] for share in range(shares)], axis=0)
        for level in range(parts.shape[1])
    ]
    gram = functools.reduce(jnp.add, [gram_of(z) for z in whole])
    own = whole[0]
    for level in range(1, len(whole)):
        own = jnp.where(lax.axis_index("depth") == level, whole[level], own)
    three[...] = times(orth_factor(gram), own) * scale


def own_rows(axis, size, length):
    down = lax.broadcasted_iota(jnp.int32, (size, length), 0)
    across = lax.broadcasted_iota(jnp.int32, (size, length), 1)
    return (across == down + lax.axis_index(axis) * size).astype(jnp.float32)


def halves_side_by_side(block):
    half = block.shape[0] // 2
    return jnp.concatenate([block[:half], block[half:]], axis=1)


def halves_stacked(blocks):
    count, half, width = blocks.shape
    width //= 2
    pairs = jnp.stack([blocks[:, :, :width], blocks[:, :, width:]], axis=1)
    return pairs.reshape(count * 2 * half, width)


def body(tensor, start_one, start_two, start_three):
    size_one, size_two, size_three = tensor.shape
    rank_one = start_one.shape[1]
    rank_two = start_two.shape[1]
    rank_three = start_three.shape[1]
    rows, cols, depth = (lax.axis_size(name) for name in ("rows", "cols", "depth"))
    length_one, length_two, length_three = size_one * rows, size_two * cols, size_three * depth
    half_team = CLASSES // 2

    def core_of(half, row, col):
        return (half + row + col) % depth

    blocks = [
        [(row * cols + col) * depth + core_of(half, row, col) for col in range(cols) for half in range(depth)]
        for row in range(rows)
    ]
    chips = [order[at : at + depth] for order in blocks for at in range(0, cols * depth, depth)]
    lines_of_chips = [
        [row * depth + core_of(half, row, 0) for row in range(rows)] for half in range(depth)
    ]
    teams = [
        [col * depth + core_of(half, 0, col) for col in range(first, first + CLASSES)]
        for first in range(0, cols, CLASSES)
        for half in range(depth)
    ]
    near = [
        list(range(first * depth, (first + half_team) * depth))
        for first in range(0, cols, half_team)
    ]
    far = [
        [first + at, first + half_team + at]
        for first in range(0, cols, CLASSES)
        for at in range(half_team)
    ]
    slices = rank_three // (CLASSES * depth)
    flat = tensor.reshape(size_one * size_two, size_three)

    thinned = lax.dot_general(
        start_three, flat, (((0,), (1,)), ((), ())), precision=exact_mode
    ).reshape(1, depth, CLASSES, -1, LANES)
    lines = thinned.shape[3]
    two_packed = halves_side_by_side(start_two)
    thinned = jnp.broadcast_to(
        thinned.transpose(0, 2, 1, 3, 4), (cols // CLASSES, CLASSES, depth, lines, LANES)
    ).reshape(cols * depth, lines, LANES)
    message = jnp.concatenate(
        [thinned, jnp.broadcast_to(two_packed[None], (cols * depth, *two_packed.shape))], axis=1
    )
    one_packed = halves_side_by_side(start_one)
    got, one_packed, flat = alone(
        lambda shard: lax.all_to_all(
            shard, EVERYWHERE, 0, 0, tiled=True, axis_index_groups=blocks
        ),
        message, one_packed, flat,
    )
    got = got.reshape(cols, depth, *got.shape[1:])
    own = got[:, :, :lines].sum(axis=1).reshape(cols, slices * size_one, size_two)
    own = own.transpose(1, 0, 2).reshape(slices * size_one, length_two)
    two_old = halves_stacked(got[:, 0, lines:])

    got = lax.all_gather(
        jnp.concatenate([own, one_packed], axis=0),
        ("rows", "depth"),
        axis_index_groups=lines_of_chips,
    )

    cut = (size_one, slices)
    z_part = kernel_call(
        functools.partial(first_mode, *cut), (rank_one, length_one), got, two_old
    )
    z_part = lax.all_gather(z_part, ("cols", "depth"), axis_index_groups=near).sum(axis=0)
    z_parts = lax.all_gather(z_part, "cols", axis_index_groups=far)

    one, projected = kernel_call(
        functools.partial(to_second, *cut),
        ((rank_one, length_one), (slices * rank_one, length_two)),
        z_parts,
        got,
    )
    projected = lax.all_gather(projected, ("cols", "depth"), axis_index_groups=teams)
    projected = projected.reshape(-1, length_two)
    z_part = kernel_call(second_mode, (rank_two, length_two), projected, two_old)
    z_parts = lax.all_gather(z_part, "depth")

    half = projected.shape[0] // rank_one
    two, one_own, two_own, spread = kernel_call(
        to_third,
        (
            (rank_two, length_two),
            (size_one, rank_one),
            (size_two, rank_two),
            (half * size_one, size_two),
        ),
        z_parts,
        projected,
        one,
    )
    spread = lax.all_gather(spread.reshape(half, -1), EVERYWHERE, axis_index_groups=chips)
    spread = spread.reshape(rank_three, -1)
    shares = jnp.broadcast_to(
        mul(spread, flat).reshape(1, half_team, -1, size_three),
        (cols // half_team, half_team, rank_three // half_team, size_three),
    ).reshape(cols, -1, size_three)
    z_part, two, projected, one_own, two_own = alone(
        lambda shard: lax.all_to_all(shard, "cols", 0, 0, tiled=True),
        shares, two, projected, one_own, two_own,
    )
    z_part = from_everyone(z_part.sum(axis=0), "rows").sum(axis=0)
    z_parts = lax.all_gather(z_part, ("cols", "depth"), axis_index_groups=near)
    three = kernel_call(
        functools.partial(last_orth, math.sqrt(length_three)),
        (rank_three, size_three),
        z_parts.reshape(half_team, depth, -1, size_three),
    )

    core = lax.all_gather(
        mul(two, projected.T), EVERYWHERE, axis_index_groups=chips
    )
    core = core.reshape(depth, rank_two, -1, rank_one)
    core = core.transpose(3, 1, 0, 2).reshape(rank_one, rank_two, rank_three)
    return (
        one_own * math.sqrt(length_one),
        two_own * math.sqrt(length_two),
        three.T,
        core,
    )


def solution(mesh):
    in_specs = (
        P(("groups", "rows"), "cols", "depth"),
        P(("groups", "rows"), None),
        P(("groups", "cols"), None),
        P(("groups", "depth"), None),
    )
    out_specs = (
        P(("groups", "rows"), None),
        P(("groups", "cols"), None),
        P(("groups", "depth"), None),
        P("groups", None, None),
    )
    return jax.shard_map(body, mesh=mesh, in_specs=in_specs, out_specs=out_specs, check_vma=False)
```

```python
import functools
import math

import jax
import jax.numpy as jnp
from jax import lax
from jax.experimental import pallas as pl
from jax.experimental.pallas import tpu as pltpu
from jax.sharding import PartitionSpec as P

NEWTON = 3
LANES = 128
CLASSES = 4
EVERYWHERE = ("rows", "cols", "depth")
KERNEL_BYTES = 8 * 2**20
exact_mode = lax.Precision.HIGHEST


def mul(left, right):
    return jnp.dot(left, right, precision=exact_mode)


def from_everyone(shard, axis):
    peers = lax.axis_size(axis)
    return lax.all_to_all(
        jnp.broadcast_to(shard[None], (peers, *shard.shape)), axis, 0, 0, tiled=True
    )


def alone(operation, shard, *others):
    shard, others = lax.optimization_barrier((shard, others))
    return lax.optimization_barrier((operation(shard), *others))


def mul_nt(left, right):
    return lax.dot_general(left, right, (((1,), (1,)), ((), ())), precision=exact_mode)


def mul_tn(left, right):
    return lax.dot_general(left, right, (((0,), (0,)), ((), ())), precision=exact_mode)


def orth_factor(gram):
    down = lax.broadcasted_iota(jnp.int32, gram.shape, 0)
    across = lax.broadcasted_iota(jnp.int32, gram.shape, 1)
    identity = (down == across).astype(jnp.float32)
    total = jnp.sum(gram * identity, keepdims=True) + 1e-06
    gram = gram / total
    factor = None
    for step in range(NEWTON):
        move = 1.5 * identity - 0.5 * gram
        factor = move if factor is None else mul(factor, move)
        if step + 1 < NEWTON:
            gram = mul(mul(move, gram), move)
    return factor / jnp.sqrt(total)


def kernel_call(kernel, shapes, *operands):
    one = not isinstance(shapes[0], tuple)
    whole = pl.BlockSpec(memory_space=pltpu.VMEM)
    outs = [jax.ShapeDtypeStruct(shape, jnp.float32) for shape in ([shapes] if one else shapes)]
    return pl.pallas_call(
        kernel,
        out_shape=outs[0] if one else outs,
        in_specs=[whole] * len(operands),
        out_specs=whole if one else [whole] * len(outs),
        compiler_params=pltpu.CompilerParams(vmem_limit_bytes=KERNEL_BYTES),
    )(*operands)


def class_matrices(got, size_one, slices):
    return [
        got[:, c * size_one : (c + 1) * size_one, :].reshape(-1, got.shape[2])
        for c in range(slices)
    ]


def first_mode(size_one, slices, got, two_old, z_part):
    packed = got[:, slices * size_one :, :]
    width = packed.shape[2] // 2
    one_old = jnp.stack([packed[:, :, :width], packed[:, :, width:]], axis=1)
    one_old = one_old.reshape(-1, width)
    two = two_old[...]
    none = jnp.zeros_like(two)
    twice = jnp.concatenate(
        [jnp.concatenate([two, none], axis=1), jnp.concatenate([none, two], axis=1)], axis=0
    )
    whole = class_matrices(got, size_one, slices)
    pairs = [jnp.concatenate(whole[c : c + 2], axis=1) for c in range(0, slices, 2)]
    unfolded = jnp.concatenate([mul(pair, twice) for pair in pairs], axis=1)
    z_part[...] = mul_nt(mul(one_old.T, unfolded), unfolded)


def to_second(size_one, slices, z_parts, got, one, projected):
    z = jnp.sum(z_parts[...], axis=0)
    new = mul(orth_factor(mul_nt(z, z)), z)
    one[...] = new
    rank = new.shape[0]
    width = got.shape[2]
    wide = mul(new, jnp.concatenate(class_matrices(got, size_one, slices), axis=1))
    for c in range(slices):
        projected[c * rank : (c + 1) * rank, :] = wide[:, c * width : (c + 1) * width]


def second_mode(projected, two_old, z_part):
    z_part[...] = mul(mul_nt(two_old[...].T, projected[...]), projected[...])


def to_third(z_parts, projected, one, two, one_own, two_own, spread):
    z = jnp.sum(z_parts[...], axis=0)
    new = mul(orth_factor(mul_nt(z, z)), z)
    two[...] = new
    rank, length_one = one.shape
    length_two = new.shape[1]
    size_one, size_two = one_own.shape[0], two_own.shape[0]
    first = mul_nt(own_rows("rows", size_one, length_one), one[...])
    second = mul_nt(own_rows("cols", size_two, length_two), new)
    one_own[...] = first
    two_own[...] = second
    held = projected.shape[0] // rank
    wide = jnp.concatenate(
        [projected[c * rank : (c + 1) * rank, :] for c in range(held)], axis=1
    )
    wide = mul(first, wide)
    tall = jnp.concatenate(
        [wide[:, c * length_two : (c + 1) * length_two] for c in range(held)], axis=0
    )
    spread[...] = mul_nt(tall, mul(second, new))


def last_orth(scale, parts, three):
    shares = parts.shape[0]
    whole = [
        jnp.concatenate([parts[share, level] for share in range(shares)], axis=0)
        for level in range(parts.shape[1])
    ]
    gram = functools.reduce(jnp.add, [mul_nt(z, z) for z in whole])
    own = whole[0]
    for level in range(1, len(whole)):
        own = jnp.where(lax.axis_index("depth") == level, whole[level], own)
    three[...] = mul(orth_factor(gram), own) * scale


def own_rows(axis, size, length):
    down = lax.broadcasted_iota(jnp.int32, (size, length), 0)
    across = lax.broadcasted_iota(jnp.int32, (size, length), 1)
    return (across == down + lax.axis_index(axis) * size).astype(jnp.float32)


def halves_side_by_side(block):
    half = block.shape[0] // 2
    return jnp.concatenate([block[:half], block[half:]], axis=1)


def halves_stacked(blocks):
    count, half, width = blocks.shape
    width //= 2
    pairs = jnp.stack([blocks[:, :, :width], blocks[:, :, width:]], axis=1)
    return pairs.reshape(count * 2 * half, width)


def body(tensor, start_one, start_two, start_three):
    size_one, size_two, size_three = tensor.shape
    rank_one = start_one.shape[1]
    rank_two = start_two.shape[1]
    rank_three = start_three.shape[1]
    rows, cols, depth = (lax.axis_size(name) for name in ("rows", "cols", "depth"))
    length_one, length_two, length_three = size_one * rows, size_two * cols, size_three * depth
    half_team = CLASSES // 2

    def core_of(half, row, col):
        return (half + row + col) % depth

    blocks = [
        [(row * cols + col) * depth + core_of(half, row, col) for col in range(cols) for half in range(depth)]
        for row in range(rows)
    ]
    chips = [order[at : at + depth] for order in blocks for at in range(0, cols * depth, depth)]
    lines_of_chips = [
        [row * depth + core_of(half, row, 0) for row in range(rows)] for half in range(depth)
    ]
    teams = [
        [col * depth + core_of(half, 0, col) for col in range(first, first + CLASSES)]
        for first in range(0, cols, CLASSES)
        for half in range(depth)
    ]
    near = [
        list(range(first * depth, (first + half_team) * depth))
        for first in range(0, cols, half_team)
    ]
    far = [
        [first + at, first + half_team + at]
        for first in range(0, cols, CLASSES)
        for at in range(half_team)
    ]
    slices = rank_three // (CLASSES * depth)
    flat = tensor.reshape(size_one * size_two, size_three)

    thinned = lax.dot_general(
        start_three, flat, (((0,), (1,)), ((), ())), precision=exact_mode
    ).reshape(1, depth, CLASSES, -1, LANES)
    lines = thinned.shape[3]
    two_packed = halves_side_by_side(start_two)
    thinned = jnp.broadcast_to(
        thinned.transpose(0, 2, 1, 3, 4), (cols // CLASSES, CLASSES, depth, lines, LANES)
    ).reshape(cols * depth, lines, LANES)
    message = jnp.concatenate(
        [thinned, jnp.broadcast_to(two_packed[None], (cols * depth, *two_packed.shape))], axis=1
    )
    one_packed = halves_side_by_side(start_one)
    got, one_packed, flat = alone(
        lambda shard: lax.all_to_all(
            shard, EVERYWHERE, 0, 0, tiled=True, axis_index_groups=blocks
        ),
        message, one_packed, flat,
    )
    got = got.reshape(cols, depth, *got.shape[1:])
    own = got[:, :, :lines].sum(axis=1).reshape(cols, slices * size_one, size_two)
    own = own.transpose(1, 0, 2).reshape(slices * size_one, length_two)
    two_old = halves_stacked(got[:, 0, lines:])

    got = lax.all_gather(
        jnp.concatenate([own, one_packed], axis=0),
        ("rows", "depth"),
        axis_index_groups=lines_of_chips,
    )

    cut = (size_one, slices)
    z_part = kernel_call(
        functools.partial(first_mode, *cut), (rank_one, length_one), got, two_old
    )
    z_part = lax.all_gather(z_part, ("cols", "depth"), axis_index_groups=near).sum(axis=0)
    z_parts = lax.all_gather(z_part, "cols", axis_index_groups=far)

    one, projected = kernel_call(
        functools.partial(to_second, *cut),
        ((rank_one, length_one), (slices * rank_one, length_two)),
        z_parts,
        got,
    )
    projected = lax.all_gather(projected, ("cols", "depth"), axis_index_groups=teams)
    projected = projected.reshape(-1, length_two)
    z_part = kernel_call(second_mode, (rank_two, length_two), projected, two_old)
    z_parts = lax.all_gather(z_part, "depth")

    half = projected.shape[0] // rank_one
    two, one_own, two_own, spread = kernel_call(
        to_third,
        (
            (rank_two, length_two),
            (size_one, rank_one),
            (size_two, rank_two),
            (half * size_one, size_two),
        ),
        z_parts,
        projected,
        one,
    )
    spread = lax.all_gather(spread.reshape(half, -1), EVERYWHERE, axis_index_groups=chips)
    spread = spread.reshape(rank_three, -1)
    shares = jnp.broadcast_to(
        mul(spread, flat).reshape(1, CLASSES, -1, size_three),
        (cols // CLASSES, CLASSES, rank_three // CLASSES, size_three),
    ).reshape(cols, -1, size_three)
    z_part, two, projected, one_own, two_own = alone(
        lambda shard: lax.all_to_all(shard, "cols", 0, 0, tiled=True),
        shares, two, projected, one_own, two_own,
    )
    z_part = from_everyone(z_part.sum(axis=0), "rows").sum(axis=0)
    core = lax.all_gather(
        mul(two, projected.T), EVERYWHERE, axis_index_groups=chips
    )
    core = core.reshape(depth, rank_two, -1, rank_one)
    core = core.transpose(3, 1, 0, 2).reshape(rank_one, rank_two, rank_three)
    one_own = one_own * math.sqrt(length_one)
    two_own = two_own * math.sqrt(length_two)
    z_parts, core, one_own, two_own = alone(
        lambda shard: lax.all_to_all(
            jnp.broadcast_to(shard[None], (CLASSES * depth, *shard.shape)),
            ("cols", "depth"),
            0,
            0,
            tiled=True,
            axis_index_groups=[
                list(range(first, first + CLASSES * depth))
                for first in range(0, cols * depth, CLASSES * depth)
            ],
        ),
        z_part, core, one_own, two_own,
    )
    three = kernel_call(
        functools.partial(last_orth, math.sqrt(length_three)),
        (rank_three, size_three),
        z_parts.reshape(CLASSES, depth, -1, size_three),
    )
    return one_own, two_own, three.T, core


def solution(mesh):
    in_specs = (
        P(("groups", "rows"), "cols", "depth"),
        P(("groups", "rows"), None),
        P(("groups", "cols"), None),
        P(("groups", "depth"), None),
    )
    out_specs = (
        P(("groups", "rows"), None),
        P(("groups", "cols"), None),
        P(("groups", "depth"), None),
        P("groups", None, None),
    )
    return jax.shard_map(body, mesh=mesh, in_specs=in_specs, out_specs=out_specs, check_vma=False)
```

```python
import functools
import math

import jax
import jax.numpy as jnp
from jax import lax
from jax.experimental import pallas as pl
from jax.experimental.pallas import tpu as pltpu
from jax.sharding import PartitionSpec as P

NEWTON = 3
LANES = 128
CLASSES = 4
EVERYWHERE = ("rows", "cols", "depth")
KERNEL_BYTES = 8 * 2**20
exact_mode = lax.Precision.HIGHEST


def mul(left, right):
    return jnp.dot(left, right, precision=exact_mode)


def from_everyone(shard, axis):
    peers = lax.axis_size(axis)
    return lax.all_to_all(
        jnp.broadcast_to(shard[None], (peers, *shard.shape)), axis, 0, 0, tiled=True
    )


def alone(operation, shard, *others):
    shard, others = lax.optimization_barrier((shard, others))
    return lax.optimization_barrier((operation(shard), *others))


def mul_nt(left, right):
    return lax.dot_general(left, right, (((1,), (1,)), ((), ())), precision=exact_mode)


def mul_tn(left, right):
    return lax.dot_general(left, right, (((0,), (0,)), ((), ())), precision=exact_mode)


def orth_factor(gram):
    down = lax.broadcasted_iota(jnp.int32, gram.shape, 0)
    across = lax.broadcasted_iota(jnp.int32, gram.shape, 1)
    identity = (down == across).astype(jnp.float32)
    total = jnp.sum(gram * identity, keepdims=True) + 1e-06
    gram = gram / total
    factor = None
    for step in range(NEWTON):
        move = 1.5 * identity - 0.5 * gram
        factor = move if factor is None else mul(factor, move)
        if step + 1 < NEWTON:
            gram = mul(mul(move, gram), move)
    return factor / jnp.sqrt(total)


def kernel_call(kernel, shapes, *operands):
    one = not isinstance(shapes[0], tuple)
    whole = pl.BlockSpec(memory_space=pltpu.VMEM)
    outs = [jax.ShapeDtypeStruct(shape, jnp.float32) for shape in ([shapes] if one else shapes)]
    return pl.pallas_call(
        kernel,
        out_shape=outs[0] if one else outs,
        in_specs=[whole] * len(operands),
        out_specs=whole if one else [whole] * len(outs),
        compiler_params=pltpu.CompilerParams(vmem_limit_bytes=KERNEL_BYTES),
    )(*operands)


def class_matrices(got, size_one, slices):
    return [
        got[:, c * size_one : (c + 1) * size_one, :].reshape(-1, got.shape[2])
        for c in range(slices)
    ]


def first_mode(size_one, slices, got, two_old, z_part):
    packed = got[:, slices * size_one :, :]
    width = packed.shape[2] // 2
    one_old = jnp.stack([packed[:, :, :width], packed[:, :, width:]], axis=1)
    one_old = one_old.reshape(-1, width)
    two = two_old[...]
    none = jnp.zeros_like(two)
    twice = jnp.concatenate(
        [jnp.concatenate([two, none], axis=1), jnp.concatenate([none, two], axis=1)], axis=0
    )
    whole = class_matrices(got, size_one, slices)
    pairs = [jnp.concatenate(whole[c : c + 2], axis=1) for c in range(0, slices, 2)]
    unfolded = jnp.concatenate([mul(pair, twice) for pair in pairs], axis=1)
    z_part[...] = mul_nt(mul(one_old.T, unfolded), unfolded)


def to_second(size_one, slices, z_parts, got, one, projected):
    z = jnp.sum(z_parts[...], axis=0)
    new = mul(orth_factor(mul_nt(z, z)), z)
    one[...] = new
    rank = new.shape[0]
    width = got.shape[2]
    wide = mul(new, jnp.concatenate(class_matrices(got, size_one, slices), axis=1))
    for c in range(slices):
        projected[c * rank : (c + 1) * rank, :] = wide[:, c * width : (c + 1) * width]


def second_mode(projected, two_old, z_part):
    z_part[...] = mul(mul_nt(two_old[...].T, projected[...]), projected[...])


def to_third(z_parts, projected, one, two, one_own, two_own, spread):
    z = jnp.sum(z_parts[...], axis=0)
    new = mul(orth_factor(mul_nt(z, z)), z)
    two[...] = new
    rank, length_one = one.shape
    length_two = new.shape[1]
    size_one, size_two = one_own.shape[0], two_own.shape[0]
    first = mul_nt(own_rows("rows", size_one, length_one), one[...])
    second = mul_nt(own_rows("cols", size_two, length_two), new)
    one_own[...] = first
    two_own[...] = second
    held = projected.shape[0] // rank
    wide = jnp.concatenate(
        [projected[c * rank : (c + 1) * rank, :] for c in range(held)], axis=1
    )
    wide = mul(first, wide)
    tall = jnp.concatenate(
        [wide[:, c * length_two : (c + 1) * length_two] for c in range(held)], axis=0
    )
    spread[...] = mul_nt(tall, mul(second, new))


def last_orth(scale, parts, three):
    shares = parts.shape[0]
    whole = [
        jnp.concatenate([parts[share, level] for share in range(shares)], axis=0)
        for level in range(parts.shape[1])
    ]
    gram = functools.reduce(jnp.add, [mul_nt(z, z) for z in whole])
    own = whole[0]
    for level in range(1, len(whole)):
        own = jnp.where(lax.axis_index("depth") == level, whole[level], own)
    three[...] = mul(orth_factor(gram), own) * scale


def own_rows(axis, size, length):
    down = lax.broadcasted_iota(jnp.int32, (size, length), 0)
    across = lax.broadcasted_iota(jnp.int32, (size, length), 1)
    return (across == down + lax.axis_index(axis) * size).astype(jnp.float32)


def halves_side_by_side(block):
    half = block.shape[0] // 2
    return jnp.concatenate([block[:half], block[half:]], axis=1)


def halves_stacked(blocks):
    count, half, width = blocks.shape
    width //= 2
    pairs = jnp.stack([blocks[:, :, :width], blocks[:, :, width:]], axis=1)
    return pairs.reshape(count * 2 * half, width)


def body(tensor, start_one, start_two, start_three):
    size_one, size_two, size_three = tensor.shape
    rank_one = start_one.shape[1]
    rank_two = start_two.shape[1]
    rank_three = start_three.shape[1]
    rows, cols, depth = (lax.axis_size(name) for name in ("rows", "cols", "depth"))
    length_one, length_two, length_three = size_one * rows, size_two * cols, size_three * depth
    half_team = CLASSES // 2

    def core_of(half, row, col):
        return (half + row + col) % depth

    blocks = [
        [(row * cols + col) * depth + core_of(half, row, col) for col in range(cols) for half in range(depth)]
        for row in range(rows)
    ]
    chips = [order[at : at + depth] for order in blocks for at in range(0, cols * depth, depth)]
    lines_of_chips = [
        [row * depth + core_of(half, row, 0) for row in range(rows)] for half in range(depth)
    ]
    teams = [
        [col * depth + core_of(half, 0, col) for col in range(first, first + CLASSES)]
        for first in range(0, cols, CLASSES)
        for half in range(depth)
    ]
    near = [
        list(range(first * depth, (first + half_team) * depth))
        for first in range(0, cols, half_team)
    ]
    far = []
    for last in range(half_team - 1, cols, half_team):
        pair = [last, (last + 1) % cols]
        far.append(pair if last % CLASSES < half_team else pair[::-1])
    slices = rank_three // (CLASSES * depth)
    flat = tensor.reshape(size_one * size_two, size_three)

    thinned = lax.dot_general(
        start_three, flat, (((0,), (1,)), ((), ())), precision=exact_mode
    ).reshape(1, depth, CLASSES, -1, LANES)
    lines = thinned.shape[3]
    two_packed = halves_side_by_side(start_two)
    thinned = jnp.broadcast_to(
        thinned.transpose(0, 2, 1, 3, 4), (cols // CLASSES, CLASSES, depth, lines, LANES)
    ).reshape(cols * depth, lines, LANES)
    message = jnp.concatenate(
        [thinned, jnp.broadcast_to(two_packed[None], (cols * depth, *two_packed.shape))], axis=1
    )
    one_packed = halves_side_by_side(start_one)
    got, one_packed, flat = alone(
        lambda shard: lax.all_to_all(
            shard, EVERYWHERE, 0, 0, tiled=True, axis_index_groups=blocks
        ),
        message, one_packed, flat,
    )
    got = got.reshape(cols, depth, *got.shape[1:])
    own = got[:, :, :lines].sum(axis=1).reshape(cols, slices * size_one, size_two)
    own = own.transpose(1, 0, 2).reshape(slices * size_one, length_two)
    two_old = halves_stacked(got[:, 0, lines:])

    got = lax.all_gather(
        jnp.concatenate([own, one_packed], axis=0),
        ("rows", "depth"),
        axis_index_groups=lines_of_chips,
    )

    cut = (size_one, slices)
    z_part = kernel_call(
        functools.partial(first_mode, *cut), (rank_one, length_one), got, two_old
    )
    z_part = lax.all_gather(z_part, ("cols", "depth"), axis_index_groups=near).sum(axis=0)
    z_parts = lax.all_gather(z_part, "cols", axis_index_groups=far)

    one, projected = kernel_call(
        functools.partial(to_second, *cut),
        ((rank_one, length_one), (slices * rank_one, length_two)),
        z_parts,
        got,
    )
    projected = lax.all_gather(projected, ("cols", "depth"), axis_index_groups=teams)
    projected = projected.reshape(-1, length_two)
    z_part = kernel_call(second_mode, (rank_two, length_two), projected, two_old)
    z_parts = lax.all_gather(z_part, "depth")

    half = projected.shape[0] // rank_one
    two, one_own, two_own, spread = kernel_call(
        to_third,
        (
            (rank_two, length_two),
            (size_one, rank_one),
            (size_two, rank_two),
            (half * size_one, size_two),
        ),
        z_parts,
        projected,
        one,
    )
    spread = lax.all_gather(spread.reshape(half, -1), EVERYWHERE, axis_index_groups=chips)
    spread = spread.reshape(rank_three, -1)
    shares = jnp.broadcast_to(
        mul(spread, flat).reshape(1, half_team, -1, size_three),
        (cols // half_team, half_team, rank_three // half_team, size_three),
    ).reshape(cols, -1, size_three)
    z_part, two, projected, one_own, two_own = alone(
        lambda shard: lax.all_to_all(shard, "cols", 0, 0, tiled=True),
        shares, two, projected, one_own, two_own,
    )
    z_part = from_everyone(z_part.sum(axis=0), "rows").sum(axis=0)
    z_parts = lax.all_gather(z_part, ("cols", "depth"), axis_index_groups=near)
    three = kernel_call(
        functools.partial(last_orth, math.sqrt(length_three)),
        (rank_three, size_three),
        z_parts.reshape(half_team, depth, -1, size_three),
    )

    core = lax.all_gather(
        mul(two, projected.T), EVERYWHERE, axis_index_groups=chips
    )
    core = core.reshape(depth, rank_two, -1, rank_one)
    core = core.transpose(3, 1, 0, 2).reshape(rank_one, rank_two, rank_three)
    return (
        one_own * math.sqrt(length_one),
        two_own * math.sqrt(length_two),
        three.T,
        core,
    )


def solution(mesh):
    in_specs = (
        P(("groups", "rows"), "cols", "depth"),
        P(("groups", "rows"), None),
        P(("groups", "cols"), None),
        P(("groups", "depth"), None),
    )
    out_specs = (
        P(("groups", "rows"), None),
        P(("groups", "cols"), None),
        P(("groups", "depth"), None),
        P("groups", None, None),
    )
    return jax.shard_map(body, mesh=mesh, in_specs=in_specs, out_specs=out_specs, check_vma=False)
```

```python
import functools
import math

import jax
import jax.numpy as jnp
from jax import lax
from jax.experimental import pallas as pl
from jax.experimental.pallas import tpu as pltpu
from jax.sharding import PartitionSpec as P

NEWTON = 3
LANES = 128
CLASSES = 4
EVERYWHERE = ("rows", "cols", "depth")
KERNEL_BYTES = 8 * 2**20
exact_mode = lax.Precision.HIGHEST


def mul(left, right):
    return jnp.dot(left, right, precision=exact_mode)


def from_everyone(shard, axis):
    peers = lax.axis_size(axis)
    return lax.all_to_all(
        jnp.broadcast_to(shard[None], (peers, *shard.shape)), axis, 0, 0, tiled=True
    )


def alone(operation, shard, *others):
    shard, others = lax.optimization_barrier((shard, others))
    return lax.optimization_barrier((operation(shard), *others))


def mul_nt(left, right):
    return lax.dot_general(left, right, (((1,), (1,)), ((), ())), precision=exact_mode)


def mul_tn(left, right):
    return lax.dot_general(left, right, (((0,), (0,)), ((), ())), precision=exact_mode)


def orth_factor(gram):
    down = lax.broadcasted_iota(jnp.int32, gram.shape, 0)
    across = lax.broadcasted_iota(jnp.int32, gram.shape, 1)
    identity = (down == across).astype(jnp.float32)
    total = jnp.sum(gram * identity, keepdims=True) + 1e-06
    gram = gram / total
    factor = None
    for step in range(NEWTON):
        move = 1.5 * identity - 0.5 * gram
        factor = move if factor is None else mul(factor, move)
        if step + 1 < NEWTON:
            gram = mul(mul(move, gram), move)
    return factor / jnp.sqrt(total)


def kernel_call(kernel, shapes, *operands):
    one = not isinstance(shapes[0], tuple)
    whole = pl.BlockSpec(memory_space=pltpu.VMEM)
    outs = [jax.ShapeDtypeStruct(shape, jnp.float32) for shape in ([shapes] if one else shapes)]
    return pl.pallas_call(
        kernel,
        out_shape=outs[0] if one else outs,
        in_specs=[whole] * len(operands),
        out_specs=whole if one else [whole] * len(outs),
        compiler_params=pltpu.CompilerParams(vmem_limit_bytes=KERNEL_BYTES),
    )(*operands)


def class_matrices(got, size_one, slices):
    return [
        got[:, c * size_one : (c + 1) * size_one, :].reshape(-1, got.shape[2])
        for c in range(slices)
    ]


def first_mode(size_one, slices, got, two_old, z_part):
    packed = got[:, slices * size_one :, :]
    width = packed.shape[2] // 2
    one_old = jnp.stack([packed[:, :, :width], packed[:, :, width:]], axis=1)
    one_old = one_old.reshape(-1, width)
    two = two_old[...]
    none = jnp.zeros_like(two)
    twice = jnp.concatenate(
        [jnp.concatenate([two, none], axis=1), jnp.concatenate([none, two], axis=1)], axis=0
    )
    whole = class_matrices(got, size_one, slices)
    pairs = [jnp.concatenate(whole[c : c + 2], axis=1) for c in range(0, slices, 2)]
    unfolded = jnp.concatenate([mul(pair, twice) for pair in pairs], axis=1)
    z_part[...] = mul_nt(mul(one_old.T, unfolded), unfolded)


def to_second(size_one, slices, z_parts, got, one, projected):
    z = jnp.sum(z_parts[...], axis=0)
    new = mul(orth_factor(mul_nt(z, z)), z)
    one[...] = new
    rank = new.shape[0]
    width = got.shape[2]
    wide = mul(new, jnp.concatenate(class_matrices(got, size_one, slices), axis=1))
    for c in range(slices):
        projected[c * rank : (c + 1) * rank, :] = wide[:, c * width : (c + 1) * width]


def second_mode(projected, two_old, z_part):
    z_part[...] = mul(mul_nt(two_old[...].T, projected[...]), projected[...])


def to_third(z_parts, projected, one, two, one_own, two_own, spread):
    z = jnp.sum(z_parts[...], axis=0)
    new = mul(orth_factor(mul_nt(z, z)), z)
    two[...] = new
    rank, length_one = one.shape
    length_two = new.shape[1]
    size_one, size_two = one_own.shape[0], two_own.shape[0]
    first = mul_nt(own_rows("rows", size_one, length_one), one[...])
    second = mul_nt(own_rows("cols", size_two, length_two), new)
    one_own[...] = first
    two_own[...] = second
    held = projected.shape[0] // rank
    wide = jnp.concatenate(
        [projected[c * rank : (c + 1) * rank, :] for c in range(held)], axis=1
    )
    wide = mul(first, wide)
    tall = jnp.concatenate(
        [wide[:, c * length_two : (c + 1) * length_two] for c in range(held)], axis=0
    )
    spread[...] = mul_nt(tall, mul(second, new))


def last_orth(scale, parts, three):
    shares = parts.shape[0]
    whole = [
        jnp.concatenate([parts[share, level] for share in range(shares)], axis=0)
        for level in range(parts.shape[1])
    ]
    gram = functools.reduce(jnp.add, [mul_nt(z, z) for z in whole])
    own = whole[0]
    for level in range(1, len(whole)):
        own = jnp.where(lax.axis_index("depth") == level, whole[level], own)
    three[...] = mul(orth_factor(gram), own) * scale


def own_rows(axis, size, length):
    down = lax.broadcasted_iota(jnp.int32, (size, length), 0)
    across = lax.broadcasted_iota(jnp.int32, (size, length), 1)
    return (across == down + lax.axis_index(axis) * size).astype(jnp.float32)


def halves_side_by_side(block):
    half = block.shape[0] // 2
    return jnp.concatenate([block[:half], block[half:]], axis=1)


def halves_stacked(blocks):
    count, half, width = blocks.shape
    width //= 2
    pairs = jnp.stack([blocks[:, :, :width], blocks[:, :, width:]], axis=1)
    return pairs.reshape(count * 2 * half, width)


def body(tensor, start_one, start_two, start_three):
    size_one, size_two, size_three = tensor.shape
    rank_one = start_one.shape[1]
    rank_two = start_two.shape[1]
    rank_three = start_three.shape[1]
    rows, cols, depth = (lax.axis_size(name) for name in ("rows", "cols", "depth"))
    length_one, length_two, length_three = size_one * rows, size_two * cols, size_three * depth
    half_team = CLASSES // 2

    def core_of(half, row, col):
        return (half + row + col) % depth

    blocks = [
        [(row * cols + col) * depth + core_of(half, row, col) for col in range(cols) for half in range(depth)]
        for row in range(rows)
    ]
    chips = [order[at : at + depth] for order in blocks for at in range(0, cols * depth, depth)]
    lines_of_chips = [
        [row * depth + core_of(half, row, 0) for row in range(rows)] for half in range(depth)
    ]
    near = [
        list(range(first * depth, (first + half_team) * depth))
        for first in range(0, cols, half_team)
    ]
    far = []
    for last in range(half_team - 1, cols, half_team):
        pair = [last, (last + 1) % cols]
        far.append(pair if last % CLASSES < half_team else pair[::-1])

    def same_half(chosen):
        return [
            [col * depth + core_of(half, 0, col) for col in pair]
            for pair in chosen
            for half in range(depth)
        ]

    near_halves = same_half(
        [list(range(first, first + half_team)) for first in range(0, cols, half_team)]
    )
    far_halves = same_half(far)
    slices = rank_three // (CLASSES * depth)
    flat = tensor.reshape(size_one * size_two, size_three)

    thinned = lax.dot_general(
        start_three, flat, (((0,), (1,)), ((), ())), precision=exact_mode
    ).reshape(1, depth, CLASSES, -1, LANES)
    lines = thinned.shape[3]
    two_packed = halves_side_by_side(start_two)
    thinned = jnp.broadcast_to(
        thinned.transpose(0, 2, 1, 3, 4), (cols // CLASSES, CLASSES, depth, lines, LANES)
    ).reshape(cols * depth, lines, LANES)
    message = jnp.concatenate(
        [thinned, jnp.broadcast_to(two_packed[None], (cols * depth, *two_packed.shape))], axis=1
    )
    one_packed = halves_side_by_side(start_one)
    got, one_packed, flat = alone(
        lambda shard: lax.all_to_all(
            shard, EVERYWHERE, 0, 0, tiled=True, axis_index_groups=blocks
        ),
        message, one_packed, flat,
    )
    got = got.reshape(cols, depth, *got.shape[1:])
    own = got[:, :, :lines].sum(axis=1).reshape(cols, slices * size_one, size_two)
    own = own.transpose(1, 0, 2).reshape(slices * size_one, length_two)
    two_old = halves_stacked(got[:, 0, lines:])

    got = lax.all_gather(
        jnp.concatenate([own, one_packed], axis=0),
        ("rows", "depth"),
        axis_index_groups=lines_of_chips,
    )

    cut = (size_one, slices)
    z_part = kernel_call(
        functools.partial(first_mode, *cut), (rank_one, length_one), got, two_old
    )
    z_part = lax.all_gather(z_part, ("cols", "depth"), axis_index_groups=near).sum(axis=0)
    z_parts = lax.all_gather(z_part, "cols", axis_index_groups=far)

    one, projected = kernel_call(
        functools.partial(to_second, *cut),
        ((rank_one, length_one), (slices * rank_one, length_two)),
        z_parts,
        got,
    )
    for groups in (near_halves, far_halves):
        projected = lax.all_gather(projected, ("cols", "depth"), axis_index_groups=groups)
        projected = projected.reshape(-1, length_two)
    z_part = kernel_call(second_mode, (rank_two, length_two), projected, two_old)
    z_parts = lax.all_gather(z_part, "depth")

    half = projected.shape[0] // rank_one
    two, one_own, two_own, spread = kernel_call(
        to_third,
        (
            (rank_two, length_two),
            (size_one, rank_one),
            (size_two, rank_two),
            (half * size_one, size_two),
        ),
        z_parts,
        projected,
        one,
    )
    spread = lax.all_gather(spread.reshape(half, -1), EVERYWHERE, axis_index_groups=chips)
    spread = spread.reshape(rank_three, -1)
    shares = jnp.broadcast_to(
        mul(spread, flat).reshape(1, half_team, -1, size_three),
        (cols // half_team, half_team, rank_three // half_team, size_three),
    ).reshape(cols, -1, size_three)
    z_part, two, projected, one_own, two_own = alone(
        lambda shard: lax.all_to_all(shard, "cols", 0, 0, tiled=True),
        shares, two, projected, one_own, two_own,
    )
    z_part = from_everyone(z_part.sum(axis=0), "rows").sum(axis=0)
    z_parts = lax.all_gather(z_part, ("cols", "depth"), axis_index_groups=near)
    three = kernel_call(
        functools.partial(last_orth, math.sqrt(length_three)),
        (rank_three, size_three),
        z_parts.reshape(half_team, depth, -1, size_three),
    )

    core = lax.all_gather(
        mul(two, projected.T), EVERYWHERE, axis_index_groups=chips
    )
    core = core.reshape(depth, rank_two, -1, rank_one)
    core = core.transpose(3, 1, 0, 2).reshape(rank_one, rank_two, rank_three)
    return (
        one_own * math.sqrt(length_one),
        two_own * math.sqrt(length_two),
        three.T,
        core,
    )


def solution(mesh):
    in_specs = (
        P(("groups", "rows"), "cols", "depth"),
        P(("groups", "rows"), None),
        P(("groups", "cols"), None),
        P(("groups", "depth"), None),
    )
    out_specs = (
        P(("groups", "rows"), None),
        P(("groups", "cols"), None),
        P(("groups", "depth"), None),
        P("groups", None, None),
    )
    return jax.shard_map(body, mesh=mesh, in_specs=in_specs, out_specs=out_specs, check_vma=False)
```
